32 devices in a mesh: obs: 4 (over z), face: 8 (over y, x, core).
Axes of the slice: x: 2, y: 2, z: 4, core: 2. Of those that a mesh axis runs over, the one named last changes fastest.
Arguments:
- density: float32 [34, 8192], P(None, ('obs', 'face')), may hold values from 0.6 to 1.4
- velocity: float32 [3, 34, 8192], P(None, None, ('obs', 'face')), may hold values from -6 to 6
- pressure: float32 [34, 8192], P(None, ('obs', 'face')), may hold values from -6 to 6
- normal: float32 [3, 8192], P(None, ('obs', 'face')), may hold values from -1 to 1, as said below
- direction: float32 [32, 8, 3], P(('obs', 'face')), may hold values from -1 to 1, as said below
- weights: bfloat16 [32, 8, 768, 256], P(('obs', 'face')), may hold values from -0.21875 to 0.21875
- bin_index: int32 [32, 8], P(('obs', 'face')), may hold values from 0 to 7, as said below
- group_index: int32 [32, 8], P(('obs', 'face')), may hold values from 0 to 3
- item_count: int32 [32], P(('obs', 'face')), may hold values from 4 to 8, as said below
Outputs:
- signal: float32 [256, 1024], P('face', 'obs')
The draws below stay inside these ranges and needn't reach their ends.
Inputs may be any that keep to these rules, and one draw needn't show every extreme that they name: `bin_index`: no time block is named more than 2 times in one device's list; in every draw some device names a block 2 times among its live entries. `item_count`: some device has all 8 entries live. Each face's normal has unit length. Each entry's direction has unit length.
All inputs are finite; a program needn't handle non-finite values.
Results may differ from the reference program's by a relative error of at most 0.0029.
Values sent between devices are 32-bit elements; how exact they have to be, the bound alone decides.
A program may use at most 64 MiB of HBM per device.

```python
import math
import jax
import jax.numpy as jnp
from jax import lax

FACE_DEV = 256
OBS_GROUP = 256
WINDOW_STEPS = 32
SLOT_CAP = 2
LIST_LEN = 8
TOTAL_FACES = 8192
OBSERVERS = 1024
SAMPLES = 256
DEVICES = 32


def unit_vectors(key, count):
    first, second = jax.random.split(key)
    height = jax.random.uniform(first, (count,), jnp.float32, -1.0, 1.0)
    azimuth = jax.random.uniform(second, (count,), jnp.float32, -math.pi, math.pi)
    radius = jnp.sqrt(jnp.maximum(1.0 - height * height, 0.0))
    return (radius * jnp.cos(azimuth), radius * jnp.sin(azimuth), height)


def draw_normal(key, part):
    east, north, upward = unit_vectors(jax.random.fold_in(key, 11), TOTAL_FACES)
    return jnp.stack([east, north, upward], axis=0).astype(jnp.float32)


def draw_direction(key, part):
    devices = TOTAL_FACES // FACE_DEV
    east, north, upward = unit_vectors(jax.random.fold_in(key, 12), devices * LIST_LEN)
    return jnp.stack([east, north, upward], axis=-1).reshape(devices, LIST_LEN, 3).astype(jnp.float32)


def draw_bin_index(key, part):
    devices = TOTAL_FACES // FACE_DEV
    n_blocks = SAMPLES // WINDOW_STEPS

    def one_row(row_key):
        order_key, block_key = jax.random.split(row_key)
        order = jax.random.permutation(order_key, LIST_LEN)
        blocks = jax.random.permutation(block_key, n_blocks)
        return blocks[order // SLOT_CAP].astype(jnp.int32)
    return jax.vmap(one_row)(jax.random.split(jax.random.fold_in(key, 13), devices))


def draw_item_count(key, part):
    devices = TOTAL_FACES // FACE_DEV
    first, second, third = jax.random.split(jax.random.fold_in(key, 14), 3)
    base = jax.random.randint(first, (devices,), LIST_LEN // 2, LIST_LEN + 1)
    full = jax.random.randint(second, (devices,), 0, 8) == 0
    chosen = jax.random.randint(third, (), 0, devices)
    forced = jnp.arange(devices) == chosen
    return jnp.where(full | forced, LIST_LEN, jnp.minimum(base, LIST_LEN)).astype(jnp.int32)


def plant(array, rng, low, top_value):
    longest = array.shape.index(max(array.shape))
    spots = []
    for shift in (0, 1):
        where = [jax.random.randint(jax.random.fold_in(rng, axis), (), 0, length) for axis, length in enumerate(array.shape)]
        where[longest] = (where[longest] + shift) % array.shape[longest]
        spots.append(tuple(where))
    return array.at[spots[0]].set(low).at[spots[1]].set(top_value)


def steps_of(key, shape, cuts, smallest, high):
    level, own = 1.0, jax.random.fold_in(key, 6)
    for axis_at, parts in cuts:
        draws = jnp.exp(jax.random.uniform(jax.random.fold_in(own, axis_at), (parts,), jnp.float32, smallest / len(cuts), high / len(cuts)))
        level = level * jnp.repeat(draws, shape[axis_at] // parts).reshape([-1 if axis == axis_at else 1 for axis in range(len(shape))])
    return level


def bell_draw(own_key, extent, width, bound, cuts=(), kind=jnp.bfloat16):
    loudness = steps_of(own_key, extent, cuts, -0.22, 0.18) if cuts else 1.0
    result = jax.random.normal(own_key, extent, jnp.float32) * width * loudness
    return jnp.minimum(jnp.maximum(result, -bound), bound).astype(kind)


def setup_inputs(seed: int = 0) -> dict:
    splits = jax.random.split(jax.random.key(seed), 10)
    density = jnp.clip(0.6 + 0.79999995 * jax.random.uniform(splits[0], (WINDOW_STEPS + 2, TOTAL_FACES), jnp.float32) ** steps_of(splits[0], (WINDOW_STEPS + 2, TOTAL_FACES), ((1, 32),), -0.2, 0.2), 0.6, 1.4)
    velocity = bell_draw(splits[1], (3, WINDOW_STEPS + 2, TOTAL_FACES), 1.0, 6.0, ((2, 32),), jnp.float32)
    pressure = bell_draw(splits[2], (WINDOW_STEPS + 2, TOTAL_FACES), 1.0, 6.0, ((1, 32),), jnp.float32)
    normal = draw_normal(jax.random.fold_in(splits[9], 71), 0)
    direction = draw_direction(jax.random.fold_in(splits[9], 71), 0)
    weights = bell_draw(splits[5], (DEVICES, LIST_LEN, 3 * FACE_DEV, OBS_GROUP), (3 * FACE_DEV) ** -0.5, 0.21875, ((0, 32),))
    bin_index = draw_bin_index(jax.random.fold_in(splits[9], 71), 0)
    group_index = plant(jax.random.randint(splits[7], (DEVICES, LIST_LEN), 0, OBSERVERS // OBS_GROUP), jax.random.fold_in(splits[7], 1), 0, (OBSERVERS // OBS_GROUP) - 1).astype(jnp.int32)
    item_count = draw_item_count(jax.random.fold_in(splits[9], 71), 0)
    return dict(density=density, velocity=velocity, pressure=pressure, normal=normal, direction=direction, weights=weights, bin_index=bin_index, group_index=group_index, item_count=item_count)


def face_terms(dens, veloc, press, norms):
    normal_speed = veloc[0] * norms[0][None] + veloc[1] * norms[1][None] + veloc[2] * norms[2][None]
    flux = dens * normal_speed
    load_first = press * norms[0][None] + dens * veloc[0] * normal_speed
    load_second = press * norms[1][None] + dens * veloc[1] * normal_speed
    load_third = press * norms[2][None] + dens * veloc[2] * normal_speed
    thick = 0.5 * (flux[2:] - flux[:-2])
    return thick, load_first, load_second, load_third


def item_source(thick, load_first, load_second, load_third, heading):
    radial = heading[0] * load_first + heading[1] * load_second + heading[2] * load_third
    rate = 0.5 * (radial[2:] - radial[:-2])
    return jnp.concatenate([thick, rate, radial[1:-1]], axis=1).astype(jnp.bfloat16)


def reference(density, velocity, pressure, normal, direction, weights, bin_index, group_index, item_count):
    n_devices = weights.shape[0]
    per_device = density.shape[1] // n_devices
    rows = density.shape[0]
    dens_dev = density.reshape(rows, n_devices, per_device).transpose(1, 0, 2)
    press_dev = pressure.reshape(rows, n_devices, per_device).transpose(1, 0, 2)
    veloc_dev = velocity.reshape(3, rows, n_devices, per_device).transpose(2, 0, 1, 3)
    norms_dev = normal.reshape(3, n_devices, per_device).transpose(1, 0, 2)
    n_blocks = SAMPLES // WINDOW_STEPS
    n_groups = OBSERVERS // OBS_GROUP
    start = jnp.zeros((n_blocks, n_groups, WINDOW_STEPS, OBS_GROUP), jnp.float32)

    def device_step(signal, inputs):
        dens, veloc, press, norms, headings, matrices, blocks_of, groups_of, live_count = inputs
        thick, load_first, load_second, load_third = face_terms(dens, veloc, press, norms)
        for listed in range(LIST_LEN):
            source = item_source(thick, load_first, load_second, load_third, headings[listed])
            block = jnp.dot(source, matrices[listed], preferred_element_type=jnp.float32)
            switch = (listed < live_count).astype(jnp.float32)
            signal = signal.at[blocks_of[listed], groups_of[listed]].add(block * switch)
        return signal, None

    signal, _ = lax.scan(device_step, start, (dens_dev, veloc_dev, press_dev, norms_dev, direction, weights, bin_index, group_index, item_count))
    return signal.transpose(0, 2, 1, 3).reshape(SAMPLES, OBSERVERS)
```

```python
import functools

import jax
import jax.numpy as jnp
from jax import lax
from jax.experimental import pallas as pl
from jax.experimental.pallas import tpu as pltpu
from jax.sharding import PartitionSpec as P

MESH = pl.DeviceIdType.MESH
PLANES = 2


def loop(first, last, body):
    if last - first <= 8:
        for at in range(first, last):
            body(at)
    else:
        lax.fori_loop(first, last, lambda at, _: (body(at), _)[1], 0)


def kernel(
    n_obs, n_face, planes, cores, chunks,
    direction_in, bin_in, group_in, item_count,
    density, velocity, pressure, normal, weights,
    out,
    direction, bin_index, group_index,
    dens, veloc, press, norms, matrices, thick, rate_of, load_of, sources,
    products, labels_out, labels_in, arrived, cells, owned,
    small_sem, in_sem, weight_sem, ready, label_send, label_recv,
    send_sem, recv_sem, send_two, recv_two,
):
    my_obs, my_face = lax.axis_index("obs"), lax.axis_index("face")
    listed_total, steps = sources.shape[:2]
    part = matrices.shape[3]
    groups = n_obs // planes
    members = planes * n_face
    owners_plane = n_face // cores
    owners = planes * owners_plane
    rows = steps // owners
    total_cells = n_obs * n_face
    lanes = min(128, members * listed_total)
    per_row = lanes // listed_total
    key_blocks = members // per_row

    my_group, my_plane = my_obs // planes, lax.rem(my_obs, planes)
    me = my_plane * n_face + my_face
    my_owner = my_plane * owners_plane + my_face // cores
    is_owner = lax.rem(my_face, cores) == cores - 1
    my_cell = my_obs * n_face + my_face

    def member_device(member):
        return (my_group * planes + member // n_face, lax.rem(member, n_face))

    def owner_device(owner):
        return (
            my_group * planes + owner // owners_plane,
            lax.rem(owner, owners_plane) * cores + cores - 1,
        )

    def counterpart(shift):
        return (lax.rem(my_obs + shift * planes, n_obs), my_face)

    smalls = [
        pltpu.make_async_copy(direction_in, direction, small_sem.at[0]),
        pltpu.make_async_copy(bin_in, bin_index, small_sem.at[1]),
        pltpu.make_async_copy(group_in, group_index, small_sem.at[2]),
    ]
    loads = [
        pltpu.make_async_copy(density, dens, in_sem.at[0]),
        pltpu.make_async_copy(velocity, veloc, in_sem.at[1]),
        pltpu.make_async_copy(pressure, press, in_sem.at[2]),
        pltpu.make_async_copy(normal, norms, in_sem.at[3]),
    ]
    for copy in smalls + loads:
        copy.start()

    def weight_copy(chunk, listed):
        return pltpu.make_async_copy(
            weights.at[0, listed, :, pl.ds(chunk * part, part)],
            matrices.at[chunk, listed],
            weight_sem.at[chunk, listed],
        )

    for chunk in range(chunks):
        loop(0, listed_total, lambda listed: weight_copy(chunk, listed).start())

    barrier = pltpu.get_barrier_semaphore()

    def greet(device):
        pl.semaphore_signal(barrier, inc=1, device_id=device, device_id_type=MESH)

    @pl.when(is_owner)
    def _():
        loop(1, members, lambda shift: greet(member_device(lax.rem(me + shift, members))))
        loop(1, groups, lambda shift: greet(counterpart(shift)))

    @pl.when(jnp.logical_not(is_owner))
    def _():
        loop(0, owners, lambda owner: greet(owner_device(owner)))

    for copy in smalls:
        copy.wait()
    live_count = item_count[0]
    lane = lax.broadcasted_iota(jnp.int32, (1, 128), 1) - lax.rem(me, per_row) * listed_total
    row = jnp.zeros((1, 128), jnp.int32)
    for listed in range(listed_total):
        label = group_index[0, listed] * n_face + bin_index[0, listed] + 1
        label = jnp.where(listed < live_count, label, 0)
        row = jnp.where(lane == listed, label, row)
    labels_out[...] = row

    for copy in loads:
        copy.wait()
    n0, n1, n2 = norms[0:1], norms[1:2], norms[2:3]
    v0, v1, v2 = veloc[0], veloc[1], veloc[2]
    density_now, pressure_now = dens[...], press[...]
    normal_speed = v0 * n0 + v1 * n1 + v2 * n2
    flux = density_now * normal_speed
    thick[...] = (0.5 * (flux[2:] - flux[:-2])).astype(jnp.bfloat16)
    for c, (n, v) in enumerate(((n0, v0), (n1, v1), (n2, v2))):
        load = pressure_now * n + density_now * v * normal_speed
        rate_of[c] = 0.5 * (load[2:] - load[:-2])
        load_of[c] = load[1:-1]

    def prepare(listed):
        h0, h1, h2 = (direction[c, 0, listed] for c in range(3))
        rate = h0 * rate_of[0] + h1 * rate_of[1] + h2 * rate_of[2]
        radial = h0 * load_of[0] + h1 * load_of[1] + h2 * load_of[2]
        sources[listed] = jnp.concatenate(
            [thick[...], rate.astype(jnp.bfloat16), radial.astype(jnp.bfloat16)], axis=1
        )

    loop(0, listed_total, prepare)

    def compute(chunk):
        for listed in range(listed_total):
            weight_copy(chunk, listed).wait()
            product = jnp.dot(
                sources[listed], matrices[chunk, listed], preferred_element_type=jnp.float32
            )
            products[chunk, pl.ds(listed, steps, stride=listed_total), :] = product

    def label_copy(owner):
        return pltpu.make_async_remote_copy(
            src_ref=labels_out,
            dst_ref=labels_in.at[me],
            send_sem=label_send,
            recv_sem=label_recv,
            device_id=owner_device(owner),
            device_id_type=MESH,
        )

    def rows_of(owner):
        size = rows * listed_total
        return pl.ds(pl.multiple_of(owner * size, size), size)

    def data_copy(chunk, owner):
        return pltpu.make_async_remote_copy(
            src_ref=products.at[chunk, rows_of(owner)],
            dst_ref=arrived.at[chunk, me],
            send_sem=send_sem.at[chunk],
            recv_sem=recv_sem.at[chunk],
            device_id=owner_device(owner),
            device_id_type=MESH,
        )

    def send_all(copy_of):
        @pl.when(is_owner)
        def _():
            loop(1, owners, lambda shift: copy_of(lax.rem(my_owner + shift, owners)).start())

        @pl.when(jnp.logical_not(is_owner))
        def _():
            loop(0, owners, lambda shift: copy_of(lax.rem(my_owner + shift, owners)).start())

    compute(0)
    pl.semaphore_wait(barrier, jnp.where(is_owner, members + groups - 2, owners))

    @pl.when(is_owner)
    def _():
        for shift in range(1, groups):
            pl.semaphore_signal(
                ready, inc=1, device_id=counterpart(shift), device_id_type=MESH
            )

    send_all(label_copy)
    send_all(functools.partial(data_copy, 0))
    for chunk in range(1, chunks):
        compute(chunk)
        send_all(functools.partial(data_copy, chunk))

    def wait_bytes(ref, sem):
        pltpu.make_async_copy(ref, ref, sem).wait()

    def cell_copy(chunk, cell):
        return pltpu.make_async_remote_copy(
            src_ref=cells.at[chunk, cell],
            dst_ref=owned.at[chunk, my_group * owners + my_owner],
            send_sem=send_two.at[chunk],
            recv_sem=recv_two.at[chunk],
            device_id=(cell // n_face, lax.rem(cell, n_face)),
            device_id_type=MESH,
        )

    @pl.when(is_owner)
    def _():
        labels_in[me] = labels_out[...]
        for chunk in range(chunks):
            arrived[chunk, me] = products[chunk, rows_of(my_owner)]
        wait_bytes(labels_in.at[pl.ds(0, members - 1)], label_recv)
        cell_number = lax.broadcasted_iota(jnp.int32, (total_cells, lanes), 0) + 1
        choose = []
        for block in range(key_blocks):
            keys = jnp.sum(labels_in[block * per_row:(block + 1) * per_row], axis=0)
            choose.append((keys[:, :lanes] == cell_number).astype(jnp.bfloat16))
        choose = jnp.concatenate(choose + choose, axis=1)
        for chunk in range(chunks):
            wait_bytes(arrived.at[chunk, pl.ds(0, members - 1)], recv_sem.at[chunk])
            values = jnp.concatenate(
                [
                    arrived[chunk, :, at * listed_total:(at + 1) * listed_total, :].reshape(
                        members * listed_total, part
                    )
                    for at in range(rows)
                ],
                axis=1,
            )
            high = values.astype(jnp.bfloat16)
            low = (values - high.astype(jnp.float32)).astype(jnp.bfloat16)
            sums = jnp.dot(
                choose,
                jnp.concatenate([high, low], axis=0),
                preferred_element_type=jnp.float32,
            )
            for at in range(rows):
                cells[chunk, :, at, :] = sums[:, at * part:(at + 1) * part]
            if chunk == 0 and groups > 1:
                pl.semaphore_wait(ready, groups - 1)
            loop(
                0,
                total_cells - 1,
                lambda at: cell_copy(chunk, at + (at >= my_cell).astype(jnp.int32)).start(),
            )
            owned[chunk, my_group * owners + my_owner] = cells[chunk, my_cell]

    senders = groups * owners
    for chunk in range(chunks):
        @pl.when(is_owner)
        def _():
            wait_bytes(owned.at[chunk, pl.ds(0, senders - 1)], recv_two.at[chunk])

        @pl.when(jnp.logical_not(is_owner))
        def _():
            wait_bytes(owned.at[chunk, pl.ds(0, senders)], recv_two.at[chunk])

        for owner in range(owners):
            total = owned[chunk, owner]
            for group in range(1, groups):
                total = total + owned[chunk, group * owners + owner]
            out[owner * rows:(owner + 1) * rows, chunk * part:(chunk + 1) * part] = total

    def drain(count):
        wait_bytes(labels_in.at[pl.ds(0, count)], label_send)
        for chunk in range(chunks):
            wait_bytes(arrived.at[chunk, pl.ds(0, count)], send_sem.at[chunk])

    @pl.when(is_owner)
    def _():
        drain(owners - 1)
        for chunk in range(chunks):
            wait_bytes(cells.at[chunk, pl.ds(0, total_cells - 1)], send_two.at[chunk])

    @pl.when(jnp.logical_not(is_owner))
    def _():
        drain(owners)


def local(
    density, velocity, pressure, normal, direction, weights, bin_index, group_index, item_count
):
    n_face, n_obs = lax.axis_size("face"), lax.axis_size("obs")
    listed_total, depth, width = weights.shape[1:]
    rows, faces = density.shape
    steps = rows - 2
    chunks = max(1, width // 128)
    part = width // chunks
    planes = PLANES if n_obs % PLANES == 0 else 1
    cores = 2 if n_face % 2 == 0 else 1
    members = planes * n_face
    owners = members // cores
    groups = n_obs // planes
    total_cells = n_obs * n_face
    own_rows = steps // owners
    smem = pl.BlockSpec(memory_space=pltpu.SMEM)
    anywhere = pl.BlockSpec(memory_space=pl.ANY)
    f32, i32 = jnp.float32, jnp.int32
    dma = pltpu.SemaphoreType.DMA
    return pl.pallas_call(
        functools.partial(kernel, n_obs, n_face, planes, cores, chunks),
        out_shape=pltpu.VMEM((steps, width), f32),
        in_specs=[anywhere] * 3 + [smem] + [anywhere] * 5,
        out_specs=pl.BlockSpec(memory_space=pltpu.VMEM),
        scratch_shapes=[
            pltpu.SMEM((3, 1, listed_total), f32),
            pltpu.SMEM((1, listed_total), i32),
            pltpu.SMEM((1, listed_total), i32),
            pltpu.VMEM((rows, faces), f32),
            pltpu.VMEM((3, rows, faces), f32),
            pltpu.VMEM((rows, faces), f32),
            pltpu.VMEM((3, faces), f32),
            pltpu.VMEM((chunks, listed_total, depth, part), jnp.bfloat16),
            pltpu.VMEM((steps, faces), jnp.bfloat16),
            pltpu.VMEM((3, steps, faces), f32),
            pltpu.VMEM((3, steps, faces), f32),
            pltpu.VMEM((listed_total, steps, depth), jnp.bfloat16),
            pltpu.VMEM((chunks, steps * listed_total, part), f32),
            pltpu.VMEM((1, 128), i32),
            pltpu.VMEM((members, 1, 128), i32),
            pltpu.VMEM((chunks, members, own_rows * listed_total, part), f32),
            pltpu.VMEM((chunks, total_cells, own_rows, part), f32),
            pltpu.VMEM((chunks, groups * owners, own_rows, part), f32),
            dma((3,)),
            dma((4,)),
            dma((chunks, listed_total)),
            pltpu.SemaphoreType.REGULAR,
            dma,
            dma,
            dma((chunks,)),
            dma((chunks,)),
            dma((chunks,)),
            dma((chunks,)),
        ],
        compiler_params=pltpu.CompilerParams(
            collective_id=0, has_side_effects=True
        ),
    )(
        jnp.transpose(direction, (2, 0, 1)), bin_index, group_index, item_count,
        density, velocity, pressure, normal, weights,
    )


def solution(mesh):
    placed = (
        P(None, ("obs", "face")),
        P(None, None, ("obs", "face")),
        P(None, ("obs", "face")),
        P(None, ("obs", "face")),
        P(("obs", "face"), None, None),
        P(("obs", "face"), None, None, None),
        P(("obs", "face"), None),
        P(("obs", "face"), None),
        P(("obs", "face")),
    )
    return jax.shard_map(
        local, mesh=mesh, in_specs=placed, out_specs=P("face", "obs"), check_vma=False
    )
```

```python
import functools

import jax
import jax.numpy as jnp
from jax import lax
from jax.experimental import pallas as pl
from jax.experimental.pallas import tpu as pltpu
from jax.sharding import PartitionSpec as P

MESH = pl.DeviceIdType.MESH
BATCH = 8
PLANES = 1


def loop(first, last, body):
    if last - first <= 8:
        for at in range(first, last):
            body(at)
    else:
        lax.fori_loop(first, last, lambda at, _: (body(at), _)[1], 0)


def kernel(
    n_obs, n_face, planes, cores, chunks,
    direction_in, bin_in, group_in, item_count,
    density, velocity, pressure, normal, weights,
    out,
    direction, bin_index, group_index,
    dens, veloc, press, norms, matrices, thick, rate_of, load_of, sources,
    products, labels_out, labels_in, arrived, cells, owned,
    small_sem, in_sem, weight_sem, ready, label_send, label_recv,
    send_sem, recv_sem, send_two, recv_two,
):
    my_obs, my_face = lax.axis_index("obs"), lax.axis_index("face")
    listed_total, steps = sources.shape[:2]
    part = matrices.shape[3]
    groups = n_obs // planes
    members = planes * n_face
    owners_plane = n_face // cores
    owners = planes * owners_plane
    rows = steps // owners
    total_cells = n_obs * n_face
    lanes = min(128, members * listed_total)
    per_row = lanes // listed_total
    key_blocks = members // per_row

    my_group, my_plane = my_obs // planes, lax.rem(my_obs, planes)
    me = my_plane * n_face + my_face
    my_owner = my_plane * owners_plane + my_face // cores
    is_owner = lax.rem(my_face, cores) == cores - 1
    my_cell = my_obs * n_face + my_face

    def member_device(member):
        return (my_group * planes + member // n_face, lax.rem(member, n_face))

    def owner_device(owner):
        return (
            my_group * planes + owner // owners_plane,
            lax.rem(owner, owners_plane) * cores + cores - 1,
        )

    def counterpart(shift):
        return (lax.rem(my_obs + shift * planes, n_obs), my_face)

    smalls = [
        pltpu.make_async_copy(direction_in, direction, small_sem.at[0]),
        pltpu.make_async_copy(bin_in, bin_index, small_sem.at[1]),
        pltpu.make_async_copy(group_in, group_index, small_sem.at[2]),
    ]
    loads = [
        pltpu.make_async_copy(density, dens, in_sem.at[0]),
        pltpu.make_async_copy(velocity, veloc, in_sem.at[1]),
        pltpu.make_async_copy(pressure, press, in_sem.at[2]),
        pltpu.make_async_copy(normal, norms, in_sem.at[3]),
    ]
    for copy in smalls + loads:
        copy.start()

    def weight_copy(chunk, listed):
        return pltpu.make_async_copy(
            weights.at[0, listed, :, pl.ds(chunk * part, part)],
            matrices.at[chunk, listed],
            weight_sem.at[chunk, listed],
        )

    for chunk in range(chunks):
        loop(0, listed_total, lambda listed: weight_copy(chunk, listed).start())

    barrier = pltpu.get_barrier_semaphore()

    def greet(device):
        pl.semaphore_signal(barrier, inc=1, device_id=device, device_id_type=MESH)

    @pl.when(is_owner)
    def _():
        loop(1, members, lambda shift: greet(member_device(lax.rem(me + shift, members))))
        loop(1, groups, lambda shift: greet(counterpart(shift)))

    @pl.when(jnp.logical_not(is_owner))
    def _():
        loop(0, owners, lambda owner: greet(owner_device(owner)))

    for copy in smalls:
        copy.wait()
    live_count = item_count[0]
    lane = lax.broadcasted_iota(jnp.int32, (1, 128), 1) - lax.rem(me, per_row) * listed_total
    row = jnp.zeros((1, 128), jnp.int32)
    for listed in range(listed_total):
        label = group_index[0, listed] * n_face + bin_index[0, listed] + 1
        label = jnp.where(listed < live_count, label, 0)
        row = jnp.where(lane == listed, label, row)
    labels_out[...] = row

    for copy in loads:
        copy.wait()
    n0, n1, n2 = norms[0:1], norms[1:2], norms[2:3]
    v0, v1, v2 = veloc[0], veloc[1], veloc[2]
    density_now, pressure_now = dens[...], press[...]
    normal_speed = v0 * n0 + v1 * n1 + v2 * n2
    flux = density_now * normal_speed
    thick[...] = (0.5 * (flux[2:] - flux[:-2])).astype(jnp.bfloat16)
    for c, (n, v) in enumerate(((n0, v0), (n1, v1), (n2, v2))):
        load = pressure_now * n + density_now * v * normal_speed
        rate_of[c] = 0.5 * (load[2:] - load[:-2])
        load_of[c] = load[1:-1]

    def prepare(listed):
        h0, h1, h2 = (direction[c, 0, listed] for c in range(3))
        rate = h0 * rate_of[0] + h1 * rate_of[1] + h2 * rate_of[2]
        radial = h0 * load_of[0] + h1 * load_of[1] + h2 * load_of[2]
        sources[listed] = jnp.concatenate(
            [thick[...], rate.astype(jnp.bfloat16), radial.astype(jnp.bfloat16)], axis=1
        )

    loop(0, listed_total, prepare)

    def compute(chunk):
        for first in range(0, listed_total, BATCH):
            batch = range(first, min(first + BATCH, listed_total))
            for listed in batch:
                weight_copy(chunk, listed).wait()
            results = [
                jnp.dot(
                    sources[listed], matrices[chunk, listed], preferred_element_type=jnp.float32
                )
                for listed in batch
            ]
            for listed, product in zip(batch, results):
                products[chunk, pl.ds(listed, steps, stride=listed_total), :] = product

    def label_copy(owner):
        return pltpu.make_async_remote_copy(
            src_ref=labels_out,
            dst_ref=labels_in.at[me],
            send_sem=label_send,
            recv_sem=label_recv,
            device_id=owner_device(owner),
            device_id_type=MESH,
        )

    def rows_of(owner):
        size = rows * listed_total
        return pl.ds(pl.multiple_of(owner * size, size), size)

    def data_copy(chunk, owner):
        return pltpu.make_async_remote_copy(
            src_ref=products.at[chunk, rows_of(owner)],
            dst_ref=arrived.at[chunk, me],
            send_sem=send_sem.at[chunk],
            recv_sem=recv_sem.at[chunk],
            device_id=owner_device(owner),
            device_id_type=MESH,
        )

    def send_all(copy_of):
        @pl.when(is_owner)
        def _():
            loop(1, owners, lambda shift: copy_of(lax.rem(my_owner + shift, owners)).start())

        @pl.when(jnp.logical_not(is_owner))
        def _():
            loop(0, owners, lambda shift: copy_of(lax.rem(my_owner + shift, owners)).start())

    compute(0)
    pl.semaphore_wait(barrier, jnp.where(is_owner, members + groups - 2, owners))

    @pl.when(is_owner)
    def _():
        for shift in range(1, groups):
            pl.semaphore_signal(
                ready, inc=1, device_id=counterpart(shift), device_id_type=MESH
            )

    send_all(label_copy)
    send_all(functools.partial(data_copy, 0))
    for chunk in range(1, chunks):
        compute(chunk)
        send_all(functools.partial(data_copy, chunk))

    def wait_bytes(ref, sem):
        pltpu.make_async_copy(ref, ref, sem).wait()

    def cell_copy(chunk, cell):
        return pltpu.make_async_remote_copy(
            src_ref=cells.at[chunk, cell],
            dst_ref=owned.at[chunk, my_group * owners + my_owner],
            send_sem=send_two.at[chunk],
            recv_sem=recv_two.at[chunk],
            device_id=(cell // n_face, lax.rem(cell, n_face)),
            device_id_type=MESH,
        )

    @pl.when(is_owner)
    def _():
        labels_in[me] = labels_out[...]
        for chunk in range(chunks):
            arrived[chunk, me] = products[chunk, rows_of(my_owner)]
        wait_bytes(labels_in.at[pl.ds(0, members - 1)], label_recv)
        cell_number = lax.broadcasted_iota(jnp.int32, (total_cells, lanes), 0) + 1
        choose = []
        for block in range(key_blocks):
            keys = jnp.sum(labels_in[block * per_row:(block + 1) * per_row], axis=0)
            choose.append((keys[:, :lanes] == cell_number).astype(jnp.bfloat16))
        choose = jnp.concatenate(choose + choose, axis=1)
        for chunk in range(chunks):
            wait_bytes(arrived.at[chunk, pl.ds(0, members - 1)], recv_sem.at[chunk])
            values = jnp.concatenate(
                [
                    arrived[chunk, :, at * listed_total:(at + 1) * listed_total, :].reshape(
                        members * listed_total, part
                    )
                    for at in range(rows)
                ],
                axis=1,
            )
            high = values.astype(jnp.bfloat16)
            low = (values - high.astype(jnp.float32)).astype(jnp.bfloat16)
            sums = jnp.dot(
                choose,
                jnp.concatenate([high, low], axis=0),
                preferred_element_type=jnp.float32,
            )
            for at in range(rows):
                cells[chunk, :, at, :] = sums[:, at * part:(at + 1) * part]
            if chunk == 0 and groups > 1:
                pl.semaphore_wait(ready, groups - 1)
            loop(
                0,
                total_cells - 1,
                lambda at: cell_copy(chunk, at + (at >= my_cell).astype(jnp.int32)).start(),
            )
            owned[chunk, my_group * owners + my_owner] = cells[chunk, my_cell]

    senders = groups * owners
    for chunk in range(chunks):
        @pl.when(is_owner)
        def _():
            wait_bytes(owned.at[chunk, pl.ds(0, senders - 1)], recv_two.at[chunk])

        @pl.when(jnp.logical_not(is_owner))
        def _():
            wait_bytes(owned.at[chunk, pl.ds(0, senders)], recv_two.at[chunk])

        for owner in range(owners):
            total = owned[chunk, owner]
            for group in range(1, groups):
                total = total + owned[chunk, group * owners + owner]
            out[owner * rows:(owner + 1) * rows, chunk * part:(chunk + 1) * part] = total

    def drain(count):
        wait_bytes(labels_in.at[pl.ds(0, count)], label_send)
        for chunk in range(chunks):
            wait_bytes(arrived.at[chunk, pl.ds(0, count)], send_sem.at[chunk])

    @pl.when(is_owner)
    def _():
        drain(owners - 1)
        for chunk in range(chunks):
            wait_bytes(cells.at[chunk, pl.ds(0, total_cells - 1)], send_two.at[chunk])

    @pl.when(jnp.logical_not(is_owner))
    def _():
        drain(owners)


def local(
    density, velocity, pressure, normal, direction, weights, bin_index, group_index, item_count
):
    n_face, n_obs = lax.axis_size("face"), lax.axis_size("obs")
    listed_total, depth, width = weights.shape[1:]
    rows, faces = density.shape
    steps = rows - 2
    chunks = max(1, width // 128)
    part = width // chunks
    planes = PLANES if n_obs % PLANES == 0 else 1
    cores = 2 if n_face % 2 == 0 else 1
    members = planes * n_face
    owners = members // cores
    groups = n_obs // planes
    total_cells = n_obs * n_face
    own_rows = steps // owners
    smem = pl.BlockSpec(memory_space=pltpu.SMEM)
    anywhere = pl.BlockSpec(memory_space=pl.ANY)
    f32, i32 = jnp.float32, jnp.int32
    dma = pltpu.SemaphoreType.DMA
    return pl.pallas_call(
        functools.partial(kernel, n_obs, n_face, planes, cores, chunks),
        out_shape=pltpu.VMEM((steps, width), f32),
        in_specs=[anywhere] * 3 + [smem] + [anywhere] * 5,
        out_specs=pl.BlockSpec(memory_space=pltpu.VMEM),
        scratch_shapes=[
            pltpu.SMEM((3, 1, listed_total), f32),
            pltpu.SMEM((1, listed_total), i32),
            pltpu.SMEM((1, listed_total), i32),
            pltpu.VMEM((rows, faces), f32),
            pltpu.VMEM((3, rows, faces), f32),
            pltpu.VMEM((rows, faces), f32),
            pltpu.VMEM((3, faces), f32),
            pltpu.VMEM((chunks, listed_total, depth, part), jnp.bfloat16),
            pltpu.VMEM((steps, faces), jnp.bfloat16),
            pltpu.VMEM((3, steps, faces), f32),
            pltpu.VMEM((3, steps, faces), f32),
            pltpu.VMEM((listed_total, steps, depth), jnp.bfloat16),
            pltpu.VMEM((chunks, steps * listed_total, part), f32),
            pltpu.VMEM((1, 128), i32),
            pltpu.VMEM((members, 1, 128), i32),
            pltpu.VMEM((chunks, members, own_rows * listed_total, part), f32),
            pltpu.VMEM((chunks, total_cells, own_rows, part), f32),
            pltpu.VMEM((chunks, groups * owners, own_rows, part), f32),
            dma((3,)),
            dma((4,)),
            dma((chunks, listed_total)),
            pltpu.SemaphoreType.REGULAR,
            dma,
            dma,
            dma((chunks,)),
            dma((chunks,)),
            dma((chunks,)),
            dma((chunks,)),
        ],
        compiler_params=pltpu.CompilerParams(
            collective_id=0, has_side_effects=True
        ),
    )(
        jnp.transpose(direction, (2, 0, 1)), bin_index, group_index, item_count,
        density, velocity, pressure, normal, weights,
    )


def solution(mesh):
    placed = (
        P(None, ("obs", "face")),
        P(None, None, ("obs", "face")),
        P(None, ("obs", "face")),
        P(None, ("obs", "face")),
        P(("obs", "face"), None, None),
        P(("obs", "face"), None, None, None),
        P(("obs", "face"), None),
        P(("obs", "face"), None),
        P(("obs", "face")),
    )
    return jax.shard_map(
        local, mesh=mesh, in_specs=placed, out_specs=P("face", "obs"), check_vma=False
    )
```

```python
import functools

import jax
import jax.numpy as jnp
from jax import lax
from jax.experimental import pallas as pl
from jax.experimental.pallas import tpu as pltpu
from jax.sharding import PartitionSpec as P

MESH = pl.DeviceIdType.MESH
BATCH = 8
SLOT_CAP = 2
EARLY = 2
PLANES = 1


def loop(first, last, body):
    if last - first <= 8:
        for at in range(first, last):
            body(at)
    else:
        lax.fori_loop(first, last, lambda at, _: (body(at), _)[1], 0)


def kernel(
    n_obs, n_face, planes, cores, chunks, early,
    direction_in, bin_in, group_in, item_count,
    density, velocity, pressure, normal, weights,
    out,
    direction, bin_index, group_index,
    dens, veloc, press, norms, matrices, thick, rate_of, load_of, sources,
    products, labels_out, labels_in, arrived, partial, first_cells, cells, owned,
    small_sem, in_sem, weight_sem, entered, ready, label_send, label_recv,
    send_sem, recv_sem, send_two, recv_two,
):
    my_obs, my_face = lax.axis_index("obs"), lax.axis_index("face")
    listed_total, steps = sources.shape[:2]
    part = matrices[0].shape[2]
    groups = n_obs // planes
    members = planes * n_face
    owners_plane = n_face // cores
    owners = planes * owners_plane
    rows = steps // owners
    total_cells = n_obs * n_face
    waves, half = products.shape[1], listed_total // products.shape[1]
    fold = max(1, 8 // half)
    tile = fold * half
    tiles = rows // fold
    lanes = min(128, members * tile)
    per_row = lanes // tile
    key_blocks = members // per_row

    my_group, my_plane = my_obs // planes, lax.rem(my_obs, planes)
    me = my_plane * n_face + my_face
    my_owner = my_plane * owners_plane + my_face // cores
    is_owner = lax.rem(my_face, cores) == cores - 1
    my_cell = my_obs * n_face + my_face

    def member_device(member):
        return (my_group * planes + member // n_face, lax.rem(member, n_face))

    def owner_device(owner, core=cores - 1):
        return (
            my_group * planes + owner // owners_plane,
            lax.rem(owner, owners_plane) * cores + core,
        )

    def counterpart(shift):
        return (lax.rem(my_obs + shift * planes, n_obs), my_face)

    smalls = [
        pltpu.make_async_copy(direction_in, direction, small_sem.at[0]),
        pltpu.make_async_copy(bin_in, bin_index, small_sem.at[1]),
        pltpu.make_async_copy(group_in, group_index, small_sem.at[2]),
    ]
    loads = [
        pltpu.make_async_copy(density, dens, in_sem.at[0]),
        pltpu.make_async_copy(velocity, veloc, in_sem.at[1]),
        pltpu.make_async_copy(pressure, press, in_sem.at[2]),
        pltpu.make_async_copy(normal, norms, in_sem.at[3]),
    ]
    for copy in smalls + loads:
        copy.start()

    def weight_copy(chunk, listed):
        return pltpu.make_async_copy(
            weights.at[0, listed, :, pl.ds(chunk * part, part)],
            matrices[chunk].at[listed],
            weight_sem.at[chunk, listed],
        )

    loop(0, listed_total, lambda listed: weight_copy(0, listed).start())

    barrier = pltpu.get_barrier_semaphore()

    def tell(semaphore, device):
        pl.semaphore_signal(semaphore, inc=1, device_id=device, device_id_type=MESH)

    def greet(device):
        tell(barrier, device)

    @pl.when(is_owner)
    def _():
        loop(1, owners, lambda shift: greet(owner_device(lax.rem(my_owner + shift, owners))))
        loop(1, groups, lambda shift: greet(counterpart(shift)))
        for core in range(cores - 1):
            loop(0, owners, lambda owner: greet(owner_device(owner, core)))

    for chunk in range(1, chunks):
        loop(0, listed_total, lambda listed: weight_copy(chunk, listed).start())
    for copy in smalls:
        copy.wait()
    live_count = item_count[0]
    urgent, label_of = [], []
    for listed in range(listed_total):
        label = group_index[0, listed] * n_face + bin_index[0, listed]
        live = listed < live_count
        urgent.append((live & (label < early)).astype(jnp.int32))
    urgent_total = sum(urgent)
    picked = [jnp.int32(0) for _ in range(listed_total)]
    ahead = jnp.int32(0)
    for listed in range(listed_total):
        place = jnp.where(urgent[listed] == 1, ahead, urgent_total + listed - ahead)
        ahead = ahead + urgent[listed]
        picked = [jnp.where(place == at, listed, old) for at, old in enumerate(picked)]

    lane = lax.broadcasted_iota(jnp.int32, (1, 128), 1) - lax.rem(me, per_row) * tile
    for wave in range(waves):
        row = jnp.zeros((1, 128), jnp.int32)
        for at in range(half):
            listed = picked[wave * half + at]
            label = group_index[0, listed] * n_face + bin_index[0, listed] + 1
            label = jnp.where(listed < live_count, label, 0)
            for copy_at in range(fold):
                row = jnp.where(lane == copy_at * half + at, label, row)
        labels_out[wave] = row

    for copy in loads:
        copy.wait()
    n0, n1, n2 = norms[0:1], norms[1:2], norms[2:3]
    v0, v1, v2 = veloc[0], veloc[1], veloc[2]
    density_now, pressure_now = dens[...], press[...]
    normal_speed = v0 * n0 + v1 * n1 + v2 * n2
    flux = density_now * normal_speed
    thick[...] = (0.5 * (flux[2:] - flux[:-2])).astype(jnp.bfloat16)
    for c, (n, v) in enumerate(((n0, v0), (n1, v1), (n2, v2))):
        load = pressure_now * n + density_now * v * normal_speed
        rate_of[c] = 0.5 * (load[2:] - load[:-2])
        load_of[c] = load[1:-1]

    def prepare(slot):
        h0, h1, h2 = (direction[c, 0, picked[slot]] for c in range(3))
        rate = h0 * rate_of[0] + h1 * rate_of[1] + h2 * rate_of[2]
        radial = h0 * load_of[0] + h1 * load_of[1] + h2 * load_of[2]
        sources[slot] = jnp.concatenate(
            [thick[...], rate.astype(jnp.bfloat16), radial.astype(jnp.bfloat16)], axis=1
        )

    for slot in range(listed_total):
        prepare(slot)

    def compute(chunk):
        for listed in range(listed_total):
            weight_copy(chunk, listed).wait()
        for first in range(0, listed_total, BATCH):
            batch = range(first, min(first + BATCH, listed_total))
            results = [
                jnp.dot(
                    sources[slot],
                    matrices[chunk][picked[slot]],
                    preferred_element_type=jnp.float32,
                )
                for slot in batch
            ]
            for slot, product in zip(batch, results):
                wave, at = divmod(slot, half)
                products[chunk, wave, pl.ds(at, steps, stride=half), :] = product

    def label_copy(owner):
        return pltpu.make_async_remote_copy(
            src_ref=labels_out,
            dst_ref=labels_in.at[me],
            send_sem=label_send,
            recv_sem=label_recv,
            device_id=owner_device(owner),
            device_id_type=MESH,
        )

    def rows_of(owner):
        size = rows * half
        return pl.ds(pl.multiple_of(owner * size, size), size)

    def data_copy(chunk, wave, owner):
        return pltpu.make_async_remote_copy(
            src_ref=products.at[chunk, wave, rows_of(owner)],
            dst_ref=arrived.at[chunk, wave, me],
            send_sem=send_sem.at[chunk, wave],
            recv_sem=recv_sem.at[chunk, wave],
            device_id=owner_device(owner),
            device_id_type=MESH,
        )

    def send_all(copy_of):
        @pl.when(is_owner)
        def _():
            loop(1, owners, lambda shift: copy_of(lax.rem(my_owner + shift, owners)).start())

        @pl.when(jnp.logical_not(is_owner))
        def _():
            loop(0, owners, lambda shift: copy_of(lax.rem(my_owner + shift, owners)).start())

    compute(0)
    pl.semaphore_wait(barrier, jnp.where(is_owner, owners + groups - 2, owners))

    @pl.when(jnp.logical_not(is_owner))
    def _():
        loop(0, owners, lambda owner: tell(entered, owner_device(owner)))

    send_all(label_copy)
    send_all(functools.partial(data_copy, 0, 0))
    for chunk in range(1, chunks):
        compute(chunk)
        send_all(functools.partial(data_copy, chunk, 0))
    for wave in range(1, waves):
        for chunk in range(chunks):
            send_all(functools.partial(data_copy, chunk, wave))

    def wait_bytes(ref, sem):
        pltpu.make_async_copy(ref, ref, sem).wait()

    def cell_copy(source, chunk, cell):
        return pltpu.make_async_remote_copy(
            src_ref=source.at[chunk, cell],
            dst_ref=owned.at[chunk, my_group * owners + my_owner],
            send_sem=send_two.at[chunk],
            recv_sem=recv_two.at[chunk],
            device_id=(cell // n_face, cell % n_face),
            device_id_type=MESH,
        )

    def send_cells(source, chunk, first, last):
        def send(cell):
            @pl.when(cell != my_cell)
            def _():
                cell_copy(source, chunk, cell).start()

        for cell in range(first, last):
            send(cell)

        @pl.when((my_cell >= first) & (my_cell < last))
        def _():
            owned[chunk, my_group * owners + my_owner] = source[chunk, my_cell]

    @pl.when(is_owner)
    def _():
        if cores > 1:
            pl.semaphore_wait(entered, members - owners)
        for shift in range(1, groups):
            tell(ready, counterpart(shift))
        labels_in[me] = labels_out[...]
        for chunk in range(chunks):
            for wave in range(waves):
                arrived[chunk, wave, me] = products[chunk, wave, rows_of(my_owner)]
        wait_bytes(labels_in.at[pl.ds(0, members - 1)], label_recv)
        shape = (fold * total_cells, lanes)
        line = lax.broadcasted_iota(jnp.int32, shape, 0)
        place = lax.rem(lax.broadcasted_iota(jnp.int32, shape, 1), tile) // half
        chosen = []
        for wave in range(waves):
            parts = []
            for block in range(key_blocks):
                keys = jnp.sum(labels_in[block * per_row:(block + 1) * per_row, wave], axis=0)
                match = keys[:, :lanes] + place * total_cells == line + 1
                live = keys[:, :lanes] > 0
                parts.append((match & live).astype(jnp.float32).astype(jnp.bfloat16))
            chosen.append(jnp.concatenate(parts + parts, axis=1))

        for wave in range(waves):
            for chunk in range(chunks):
                wait_bytes(
                    arrived.at[chunk, wave, pl.ds(0, members - 1)], recv_sem.at[chunk, wave]
                )
                values = jnp.concatenate(
                    [
                        arrived[chunk, wave, :, at * tile:(at + 1) * tile, :].reshape(
                            members * tile, part
                        )
                        for at in range(tiles)
                    ],
                    axis=1,
                )
                high = values.astype(jnp.bfloat16)
                low = (values - high.astype(jnp.float32)).astype(jnp.bfloat16)
                sums = jnp.dot(
                    chosen[wave],
                    jnp.concatenate([high, low], axis=0),
                    preferred_element_type=jnp.float32,
                )
                if wave > 0:
                    sums = sums + partial[chunk]
                if wave < waves - 1:
                    partial[chunk] = sums
                count = total_cells if wave == waves - 1 else early
                target = cells if wave == waves - 1 else first_cells
                if wave in (0, waves - 1):
                    for at in range(rows):
                        tile_at, line_at = divmod(at, fold)
                        target[chunk, :, at, :] = sums[
                            line_at * total_cells:line_at * total_cells + count,
                            tile_at * part:(tile_at + 1) * part,
                        ]
                if wave == 0 and chunk == 0 and groups > 1:
                    pl.semaphore_wait(ready, groups - 1)
                if waves > 1 and wave == 0:
                    send_cells(first_cells, chunk, 0, early)
                if wave == waves - 1:
                    send_cells(cells, chunk, early if waves > 1 else 0, total_cells)

    senders = groups * owners
    for chunk in range(chunks):
        @pl.when(is_owner)
        def _():
            wait_bytes(owned.at[chunk, pl.ds(0, senders - 1)], recv_two.at[chunk])

        @pl.when(jnp.logical_not(is_owner))
        def _():
            wait_bytes(owned.at[chunk, pl.ds(0, senders)], recv_two.at[chunk])

        for owner in range(owners):
            total = owned[chunk, owner]
            for group in range(1, groups):
                total = total + owned[chunk, group * owners + owner]
            out[owner * rows:(owner + 1) * rows, chunk * part:(chunk + 1) * part] = total

    def drain(count):
        wait_bytes(labels_in.at[pl.ds(0, count)], label_send)
        for chunk in range(chunks):
            for wave in range(waves):
                wait_bytes(arrived.at[chunk, wave, pl.ds(0, count)], send_sem.at[chunk, wave])

    @pl.when(is_owner)
    def _():
        drain(owners - 1)
        for chunk in range(chunks):
            wait_bytes(cells.at[chunk, pl.ds(0, total_cells - 1)], send_two.at[chunk])

    @pl.when(jnp.logical_not(is_owner))
    def _():
        drain(owners)


def local(
    density, velocity, pressure, normal, direction, weights, bin_index, group_index, item_count
):
    n_face, n_obs = lax.axis_size("face"), lax.axis_size("obs")
    listed_total, depth, width = weights.shape[1:]
    rows, faces = density.shape
    steps = rows - 2
    chunks = max(1, width // 128)
    part = width // chunks
    planes = PLANES if n_obs % PLANES == 0 else 1
    cores = 2 if n_face % 2 == 0 else 1
    members = planes * n_face
    owners = members // cores
    groups = n_obs // planes
    total_cells = n_obs * n_face
    own_rows = steps // owners
    waves = 2 if listed_total % 2 == 0 and own_rows % max(1, 16 // listed_total) == 0 else 1
    half = listed_total // waves
    fold = max(1, 8 // half)
    early = min(EARLY, half // SLOT_CAP, n_face)
    smem = pl.BlockSpec(memory_space=pltpu.SMEM)
    anywhere = pl.BlockSpec(memory_space=pl.ANY)
    f32, i32 = jnp.float32, jnp.int32
    dma = pltpu.SemaphoreType.DMA
    return pl.pallas_call(
        functools.partial(kernel, n_obs, n_face, planes, cores, chunks, early),
        out_shape=pltpu.VMEM((steps, width), f32),
        in_specs=[anywhere] * 3 + [smem] + [anywhere] * 5,
        out_specs=pl.BlockSpec(memory_space=pltpu.VMEM),
        scratch_shapes=[
            pltpu.SMEM((3, 1, listed_total), f32),
            pltpu.SMEM((1, listed_total), i32),
            pltpu.SMEM((1, listed_total), i32),
            pltpu.VMEM((rows, faces), f32),
            pltpu.VMEM((3, rows, faces), f32),
            pltpu.VMEM((rows, faces), f32),
            pltpu.VMEM((3, faces), f32),
            [pltpu.VMEM((listed_total, depth, part), jnp.bfloat16)] * chunks,
            pltpu.VMEM((steps, faces), jnp.bfloat16),
            pltpu.VMEM((3, steps, faces), f32),
            pltpu.VMEM((3, steps, faces), f32),
            pltpu.VMEM((listed_total, steps, depth), jnp.bfloat16),
            pltpu.VMEM((chunks, waves, steps * half, part), f32),
            pltpu.VMEM((waves, 1, 128), i32),
            pltpu.VMEM((members, waves, 1, 128), i32),
            pltpu.VMEM((chunks, waves, members, own_rows * half, part), f32),
            pltpu.VMEM((chunks, fold * total_cells, own_rows // fold * part), f32),
            pltpu.VMEM((chunks, early, own_rows, part), f32),
            pltpu.VMEM((chunks, total_cells, own_rows, part), f32),
            pltpu.VMEM((chunks, groups * owners, own_rows, part), f32),
            dma((3,)),
            dma((4,)),
            dma((chunks, listed_total)),
            pltpu.SemaphoreType.REGULAR,
            pltpu.SemaphoreType.REGULAR,
            dma,
            dma,
            dma((chunks, waves)),
            dma((chunks, waves)),
            dma((chunks,)),
            dma((chunks,)),
        ],
        compiler_params=pltpu.CompilerParams(
            collective_id=0, has_side_effects=True
        ),
    )(
        jnp.transpose(direction, (2, 0, 1)), bin_index, group_index, item_count,
        density, velocity, pressure, normal, weights,
    )


def solution(mesh):
    placed = (
        P(None, ("obs", "face")),
        P(None, None, ("obs", "face")),
        P(None, ("obs", "face")),
        P(None, ("obs", "face")),
        P(("obs", "face"), None, None),
        P(("obs", "face"), None, None, None),
        P(("obs", "face"), None),
        P(("obs", "face"), None),
        P(("obs", "face")),
    )
    return jax.shard_map(
        local, mesh=mesh, in_specs=placed, out_specs=P("face", "obs"), check_vma=False
    )
```

```python
import functools

import jax
import jax.numpy as jnp
from jax import lax
from jax.experimental import pallas as pl
from jax.experimental.pallas import tpu as pltpu
from jax.sharding import PartitionSpec as P

MESH = pl.DeviceIdType.MESH
BATCH = 8
SLOT_CAP = 2
SPLIT = (4, 4, 2)
PLANES = 1


def loop(first, last, body):
    if last - first <= 8:
        for at in range(first, last):
            body(at)
    else:
        lax.fori_loop(first, last, lambda at, _: (body(at), _)[1], 0)


def kernel(
    n_obs, n_face, planes, cores, chunks, sizes,
    direction_in, bin_in, group_in, item_count,
    density, velocity, pressure, normal, weights,
    out,
    direction, bin_index, group_index,
    dens, veloc, press, norms, matrices, thick, rate_of, load_of, sources,
    products, labels_out, labels_in, arrived, partial, first_cells, cells, owned,
    small_sem, in_sem, weight_sem, entered, ready, label_send, label_recv,
    send_sem, recv_sem, send_two, recv_two,
):
    my_obs, my_face = lax.axis_index("obs"), lax.axis_index("face")
    listed_total, steps = sources.shape[:2]
    part = matrices[0].shape[2]
    groups = n_obs // planes
    members = planes * n_face
    owners_plane = n_face // cores
    owners = planes * owners_plane
    rows = steps // owners
    total_cells = n_obs * n_face
    waves = len(sizes)
    starts = [sum(sizes[:wave]) for wave in range(waves + 1)]
    ended = [start // SLOT_CAP for start in starts]
    folds = [max(1, 8 // size) for size in sizes]
    tiles = [fold * size for fold, size in zip(folds, sizes)]
    lanes = [min(128, members * tile) for tile in tiles]
    per_row = [wide // tile for wide, tile in zip(lanes, tiles)]

    my_group, my_plane = my_obs // planes, lax.rem(my_obs, planes)
    me = my_plane * n_face + my_face
    my_owner = my_plane * owners_plane + my_face // cores
    is_owner = lax.rem(my_face, cores) == cores - 1
    my_cell = my_obs * n_face + my_face

    def member_device(member):
        return (my_group * planes + member // n_face, lax.rem(member, n_face))

    def owner_device(owner, core=cores - 1):
        return (
            my_group * planes + owner // owners_plane,
            lax.rem(owner, owners_plane) * cores + core,
        )

    def counterpart(shift):
        return (lax.rem(my_obs + shift * planes, n_obs), my_face)

    smalls = [
        pltpu.make_async_copy(direction_in, direction, small_sem.at[0]),
        pltpu.make_async_copy(bin_in, bin_index, small_sem.at[1]),
        pltpu.make_async_copy(group_in, group_index, small_sem.at[2]),
    ]
    loads = [
        pltpu.make_async_copy(density, dens, in_sem.at[0]),
        pltpu.make_async_copy(velocity, veloc, in_sem.at[1]),
        pltpu.make_async_copy(pressure, press, in_sem.at[2]),
        pltpu.make_async_copy(normal, norms, in_sem.at[3]),
    ]
    for copy in smalls + loads:
        copy.start()

    def weight_copy(chunk, listed):
        return pltpu.make_async_copy(
            weights.at[0, listed, :, pl.ds(chunk * part, part)],
            matrices[chunk].at[listed],
            weight_sem.at[chunk, listed],
        )

    loop(0, listed_total, lambda listed: weight_copy(0, listed).start())

    barrier = pltpu.get_barrier_semaphore()

    def tell(semaphore, device):
        pl.semaphore_signal(semaphore, inc=1, device_id=device, device_id_type=MESH)

    def greet(device):
        tell(barrier, device)

    @pl.when(is_owner)
    def _():
        loop(1, owners, lambda shift: greet(owner_device(lax.rem(my_owner + shift, owners))))
        loop(1, groups, lambda shift: greet(counterpart(shift)))
        for core in range(cores - 1):
            loop(0, owners, lambda owner: greet(owner_device(owner, core)))

    for chunk in range(1, chunks):
        loop(0, listed_total, lambda listed: weight_copy(chunk, listed).start())
    for copy in smalls:
        copy.wait()
    live_count = item_count[0]
    kinds = ended[waves - 1]
    kind_of = []
    for listed in range(listed_total):
        label = group_index[0, listed] * n_face + bin_index[0, listed]
        kind_of.append(jnp.where((listed < live_count) & (label < kinds), label, kinds))
    following = [jnp.int32(0)] * (kinds + 1)
    for kind in range(1, kinds + 1):
        following[kind] = following[kind - 1] + sum(
            (of == kind - 1).astype(jnp.int32) for of in kind_of
        )
    picked = [jnp.int32(0) for _ in range(listed_total)]
    for listed in range(listed_total):
        place = jnp.int32(0)
        for kind in range(kinds + 1):
            mine = kind_of[listed] == kind
            place = jnp.where(mine, following[kind], place)
            following[kind] = following[kind] + mine.astype(jnp.int32)
        picked = [jnp.where(place == at, listed, old) for at, old in enumerate(picked)]

    lane = lax.broadcasted_iota(jnp.int32, (1, 128), 1)
    for wave in range(waves):
        lane_at = lane - lax.rem(me, per_row[wave]) * tiles[wave]
        row = jnp.zeros((1, 128), jnp.int32)
        for at in range(sizes[wave]):
            listed = picked[starts[wave] + at]
            label = group_index[0, listed] * n_face + bin_index[0, listed] + 1
            label = jnp.where(listed < live_count, label, 0)
            for copy_at in range(folds[wave]):
                row = jnp.where(lane_at == copy_at * sizes[wave] + at, label, row)
        labels_out[wave] = row

    for copy in loads:
        copy.wait()
    n0, n1, n2 = norms[0:1], norms[1:2], norms[2:3]
    v0, v1, v2 = veloc[0], veloc[1], veloc[2]
    density_now, pressure_now = dens[...], press[...]
    normal_speed = v0 * n0 + v1 * n1 + v2 * n2
    flux = density_now * normal_speed
    thick[...] = (0.5 * (flux[2:] - flux[:-2])).astype(jnp.bfloat16)
    for c, (n, v) in enumerate(((n0, v0), (n1, v1), (n2, v2))):
        load = pressure_now * n + density_now * v * normal_speed
        rate_of[c] = 0.5 * (load[2:] - load[:-2])
        load_of[c] = load[1:-1]

    def prepare(slot):
        h0, h1, h2 = (direction[c, 0, picked[slot]] for c in range(3))
        rate = h0 * rate_of[0] + h1 * rate_of[1] + h2 * rate_of[2]
        radial = h0 * load_of[0] + h1 * load_of[1] + h2 * load_of[2]
        sources[slot] = jnp.concatenate(
            [thick[...], rate.astype(jnp.bfloat16), radial.astype(jnp.bfloat16)], axis=1
        )

    for slot in range(listed_total):
        prepare(slot)

    def compute(chunk, first_wave, last_wave):
        slots = [
            (wave, at) for wave in range(first_wave, last_wave) for at in range(sizes[wave])
        ]
        for first in range(0, len(slots), BATCH):
            batch = slots[first:first + BATCH]
            results = [
                jnp.dot(
                    sources[starts[wave] + at],
                    matrices[chunk][picked[starts[wave] + at]],
                    preferred_element_type=jnp.float32,
                )
                for wave, at in batch
            ]
            for (wave, at), product in zip(batch, results):
                products[wave][chunk, pl.ds(at, steps, stride=sizes[wave]), :] = product

    def await_weights(chunk):
        for listed in range(listed_total):
            weight_copy(chunk, listed).wait()

    def label_copy(owner):
        return pltpu.make_async_remote_copy(
            src_ref=labels_out,
            dst_ref=labels_in.at[me],
            send_sem=label_send,
            recv_sem=label_recv,
            device_id=owner_device(owner),
            device_id_type=MESH,
        )

    def rows_of(wave, owner):
        size = rows * sizes[wave]
        return pl.ds(pl.multiple_of(owner * size, size), size)

    def data_copy(chunk, wave, owner):
        return pltpu.make_async_remote_copy(
            src_ref=products[wave].at[chunk, rows_of(wave, owner)],
            dst_ref=arrived[wave].at[chunk, me],
            send_sem=send_sem.at[chunk, wave],
            recv_sem=recv_sem.at[chunk, wave],
            device_id=owner_device(owner),
            device_id_type=MESH,
        )

    def send_all(copy_of):
        @pl.when(is_owner)
        def _():
            loop(1, owners, lambda shift: copy_of(lax.rem(my_owner + shift, owners)).start())

        @pl.when(jnp.logical_not(is_owner))
        def _():
            loop(0, owners, lambda shift: copy_of(lax.rem(my_owner + shift, owners)).start())

    await_weights(0)
    compute(0, 0, 1)
    pl.semaphore_wait(barrier, jnp.where(is_owner, owners + groups - 2, owners))
    send_all(functools.partial(data_copy, 0, 0))
    send_all(label_copy)

    @pl.when(jnp.logical_not(is_owner))
    def _():
        loop(0, owners, lambda owner: tell(entered, owner_device(owner)))

    compute(0, 1, waves)
    for chunk in range(1, chunks):
        await_weights(chunk)
        compute(chunk, 0, 1)
        send_all(functools.partial(data_copy, chunk, 0))
    if waves > 1:
        send_all(functools.partial(data_copy, 0, 1))
    for chunk in range(1, chunks):
        compute(chunk, 1, waves)
    for wave in range(1, waves):
        for chunk in range(chunks):
            if (wave, chunk) != (1, 0):
                send_all(functools.partial(data_copy, chunk, wave))

    def wait_bytes(ref, sem):
        pltpu.make_async_copy(ref, ref, sem).wait()

    def cell_copy(source, chunk, cell):
        return pltpu.make_async_remote_copy(
            src_ref=source.at[chunk, cell],
            dst_ref=owned.at[chunk, my_group * owners + my_owner],
            send_sem=send_two.at[chunk],
            recv_sem=recv_two.at[chunk],
            device_id=(cell // n_face, cell % n_face),
            device_id_type=MESH,
        )

    def send_cells(source, chunk, first, last):
        def send(cell):
            @pl.when(cell != my_cell)
            def _():
                cell_copy(source, chunk, cell).start()

        for cell in range(first, last):
            send(cell)

        @pl.when((my_cell >= first) & (my_cell < last))
        def _():
            owned[chunk, my_group * owners + my_owner] = source[chunk, my_cell]

    @pl.when(is_owner)
    def _():
        if cores > 1:
            pl.semaphore_wait(entered, members - owners)
        for shift in range(1, groups):
            tell(ready, counterpart(shift))
        labels_in[me] = labels_out[...]
        for chunk in range(chunks):
            for wave in range(waves):
                arrived[wave][chunk, me] = products[wave][chunk, rows_of(wave, my_owner)]
        wait_bytes(labels_in.at[pl.ds(0, members - 1)], label_recv)
        chosen = []
        for wave, (size, fold, tile) in enumerate(zip(sizes, folds, tiles)):
            shape = (fold * total_cells, lanes[wave])
            line = lax.broadcasted_iota(jnp.int32, shape, 0)
            place = lax.rem(lax.broadcasted_iota(jnp.int32, shape, 1), tile) // size
            parts = []
            for first in range(0, members, per_row[wave]):
                keys = jnp.sum(labels_in[first:first + per_row[wave], wave], axis=0)
                keys = keys[:, :lanes[wave]]
                match = (keys + place * total_cells == line + 1) & (keys > 0)
                parts.append(match.astype(jnp.float32).astype(jnp.bfloat16))
            chosen.append(jnp.concatenate(parts + parts, axis=1))

        for wave, (fold, tile) in enumerate(zip(folds, tiles)):
            last = wave == waves - 1
            begin, end = (0, total_cells) if last else ended[wave:wave + 2]
            for chunk in range(chunks):
                wait_bytes(
                    arrived[wave].at[chunk, pl.ds(0, members - 1)], recv_sem.at[chunk, wave]
                )
                values = jnp.concatenate(
                    [
                        arrived[wave][chunk, :, at * tile:(at + 1) * tile, :].reshape(
                            members * tile, part
                        )
                        for at in range(rows // fold)
                    ],
                    axis=1,
                )
                high = values.astype(jnp.bfloat16)
                low = (values - high.astype(jnp.float32)).astype(jnp.bfloat16)
                sums = jnp.dot(
                    chosen[wave],
                    jnp.concatenate([high, low], axis=0),
                    preferred_element_type=jnp.float32,
                )
                for at in range(rows):
                    tile_at, line_at = divmod(at, fold)
                    found = sums[
                        line_at * total_cells:(line_at + 1) * total_cells,
                        tile_at * part:(tile_at + 1) * part,
                    ]
                    if wave > 0:
                        found = found + partial[chunk, at]
                    if last:
                        cells[chunk, :, at, :] = found
                    else:
                        partial[chunk, at] = found
                        first_cells[chunk, begin:end, at, :] = found[begin:end]
                if wave == 0 and chunk == 0 and groups > 1:
                    pl.semaphore_wait(ready, groups - 1)
                if last:
                    send_cells(cells, chunk, kinds, max(kinds, n_face))
                else:
                    send_cells(first_cells, chunk, begin, end)
        for group in range(1, n_obs):
            for chunk in range(chunks):
                send_cells(
                    cells, chunk, max(kinds, group * n_face), (group + 1) * n_face
                )

    senders = groups * owners
    for chunk in range(chunks):
        @pl.when(is_owner)
        def _():
            wait_bytes(owned.at[chunk, pl.ds(0, senders - 1)], recv_two.at[chunk])

        @pl.when(jnp.logical_not(is_owner))
        def _():
            wait_bytes(owned.at[chunk, pl.ds(0, senders)], recv_two.at[chunk])

        for owner in range(owners):
            total = owned[chunk, owner]
            for group in range(1, groups):
                total = total + owned[chunk, group * owners + owner]
            out[owner * rows:(owner + 1) * rows, chunk * part:(chunk + 1) * part] = total

    def drain(count):
        wait_bytes(labels_in.at[pl.ds(0, count)], label_send)
        for chunk in range(chunks):
            for wave in range(waves):
                wait_bytes(arrived[wave].at[chunk, pl.ds(0, count)], send_sem.at[chunk, wave])

    @pl.when(is_owner)
    def _():
        drain(owners - 1)
        for chunk in range(chunks):
            wait_bytes(cells.at[chunk, pl.ds(0, total_cells - 1)], send_two.at[chunk])

    @pl.when(jnp.logical_not(is_owner))
    def _():
        drain(owners)


def local(
    density, velocity, pressure, normal, direction, weights, bin_index, group_index, item_count
):
    n_face, n_obs = lax.axis_size("face"), lax.axis_size("obs")
    listed_total, depth, width = weights.shape[1:]
    rows, faces = density.shape
    steps = rows - 2
    chunks = max(1, width // 128)
    part = width // chunks
    planes = PLANES if n_obs % PLANES == 0 else 1
    cores = 2 if n_face % 2 == 0 else 1
    members = planes * n_face
    owners = members // cores
    groups = n_obs // planes
    total_cells = n_obs * n_face
    own_rows = steps // owners
    sizes = tuple(listed_total // share for share in SPLIT)
    usable = all(size % SLOT_CAP == 0 and own_rows % max(1, 8 // size) == 0 for size in sizes if size)
    if sum(sizes) != listed_total or min(sizes) == 0 or not usable:
        sizes = (listed_total,)
    waves = len(sizes)
    early = max(1, sum(sizes[:-1]) // SLOT_CAP)
    smem = pl.BlockSpec(memory_space=pltpu.SMEM)
    anywhere = pl.BlockSpec(memory_space=pl.ANY)
    f32, i32 = jnp.float32, jnp.int32
    dma = pltpu.SemaphoreType.DMA
    return pl.pallas_call(
        functools.partial(kernel, n_obs, n_face, planes, cores, chunks, sizes),
        out_shape=pltpu.VMEM((steps, width), f32),
        in_specs=[anywhere] * 3 + [smem] + [anywhere] * 5,
        out_specs=pl.BlockSpec(memory_space=pltpu.VMEM),
        scratch_shapes=[
            pltpu.SMEM((3, 1, listed_total), f32),
            pltpu.SMEM((1, listed_total), i32),
            pltpu.SMEM((1, listed_total), i32),
            pltpu.VMEM((rows, faces), f32),
            pltpu.VMEM((3, rows, faces), f32),
            pltpu.VMEM((rows, faces), f32),
            pltpu.VMEM((3, faces), f32),
            [pltpu.VMEM((listed_total, depth, part), jnp.bfloat16)] * chunks,
            pltpu.VMEM((steps, faces), jnp.bfloat16),
            pltpu.VMEM((3, steps, faces), f32),
            pltpu.VMEM((3, steps, faces), f32),
            pltpu.VMEM((listed_total, steps, depth), jnp.bfloat16),
            [pltpu.VMEM((chunks, steps * size, part), f32) for size in sizes],
            pltpu.VMEM((waves, 1, 128), i32),
            pltpu.VMEM((members, waves, 1, 128), i32),
            [pltpu.VMEM((chunks, members, own_rows * size, part), f32) for size in sizes],
            pltpu.VMEM((chunks, own_rows, total_cells, part), f32),
            pltpu.VMEM((chunks, early, own_rows, part), f32),
            pltpu.VMEM((chunks, total_cells, own_rows, part), f32),
            pltpu.VMEM((chunks, groups * owners, own_rows, part), f32),
            dma((3,)),
            dma((4,)),
            dma((chunks, listed_total)),
            pltpu.SemaphoreType.REGULAR,
            pltpu.SemaphoreType.REGULAR,
            dma,
            dma,
            dma((chunks, waves)),
            dma((chunks, waves)),
            dma((chunks,)),
            dma((chunks,)),
        ],
        compiler_params=pltpu.CompilerParams(
            collective_id=0, has_side_effects=True
        ),
    )(
        jnp.transpose(direction, (2, 0, 1)), bin_index, group_index, item_count,
        density, velocity, pressure, normal, weights,
    )


def solution(mesh):
    placed = (
        P(None, ("obs", "face")),
        P(None, None, ("obs", "face")),
        P(None, ("obs", "face")),
        P(None, ("obs", "face")),
        P(("obs", "face"), None, None),
        P(("obs", "face"), None, None, None),
        P(("obs", "face"), None),
        P(("obs", "face"), None),
        P(("obs", "face")),
    )
    return jax.shard_map(
        local, mesh=mesh, in_specs=placed, out_specs=P("face", "obs"), check_vma=False
    )
```

```python
import functools

import jax
import jax.numpy as jnp
from jax import lax
from jax.experimental import pallas as pl
from jax.experimental.pallas import tpu as pltpu
from jax.sharding import PartitionSpec as P

MESH = pl.DeviceIdType.MESH
BATCH = 8
SLOT_CAP = 2
SPLIT = (4, 4, 2)
PLANES = 1


def loop(first, last, body):
    if last - first <= 8:
        for at in range(first, last):
            body(at)
    else:
        lax.fori_loop(first, last, lambda at, _: (body(at), _)[1], 0)


def kernel(
    n_obs, n_face, planes, cores, chunks, sizes,
    direction_in, bin_in, group_in, item_count,
    density, velocity, pressure, normal, weights,
    out,
    direction, bin_index, group_index,
    dens, veloc, press, norms, matrices, thick, rate_of, load_of, sources,
    products, labels_out, labels_in, arrived, partial, first_cells, cells, owned,
    small_sem, in_sem, weight_sem, entered, ready, label_send, label_recv,
    send_sem, recv_sem, send_two, recv_two,
):
    my_obs, my_face = lax.axis_index("obs"), lax.axis_index("face")
    listed_total, steps = sources.shape[:2]
    part = matrices[0].shape[2]
    groups = n_obs // planes
    members = planes * n_face
    owners_plane = n_face // cores
    owners = planes * owners_plane
    rows = steps // owners
    total_cells = n_obs * n_face
    waves = len(sizes)
    starts = [sum(sizes[:wave]) for wave in range(waves + 1)]
    ended = [start // SLOT_CAP for start in starts]
    folds = [max(1, 8 // size) for size in sizes]
    tiles = [fold * size for fold, size in zip(folds, sizes)]
    lanes = [min(128, members * tile) for tile in tiles]
    per_row = [wide // tile for wide, tile in zip(lanes, tiles)]

    my_group, my_plane = my_obs // planes, lax.rem(my_obs, planes)
    me = my_plane * n_face + my_face
    my_owner = my_plane * owners_plane + my_face // cores
    is_owner = lax.rem(my_face, cores) == cores - 1
    my_cell = my_obs * n_face + my_face

    def member_device(member):
        return (my_group * planes + member // n_face, lax.rem(member, n_face))

    def owner_device(owner, core=cores - 1):
        return (
            my_group * planes + owner // owners_plane,
            lax.rem(owner, owners_plane) * cores + core,
        )

    def counterpart(shift):
        return (lax.rem(my_obs + shift * planes, n_obs), my_face)

    smalls = [
        pltpu.make_async_copy(direction_in, direction, small_sem.at[0]),
        pltpu.make_async_copy(bin_in, bin_index, small_sem.at[1]),
        pltpu.make_async_copy(group_in, group_index, small_sem.at[2]),
    ]
    loads = [
        pltpu.make_async_copy(density, dens, in_sem.at[0]),
        pltpu.make_async_copy(velocity, veloc, in_sem.at[1]),
        pltpu.make_async_copy(pressure, press, in_sem.at[2]),
        pltpu.make_async_copy(normal, norms, in_sem.at[3]),
    ]
    for copy in smalls + loads:
        copy.start()

    def weight_copy(chunk, listed):
        return pltpu.make_async_copy(
            weights.at[0, listed, :, pl.ds(chunk * part, part)],
            matrices[chunk].at[listed],
            weight_sem.at[chunk, listed],
        )

    loop(0, listed_total, lambda listed: weight_copy(0, listed).start())

    barrier = pltpu.get_barrier_semaphore()

    def tell(semaphore, device):
        pl.semaphore_signal(semaphore, inc=1, device_id=device, device_id_type=MESH)

    def greet(device):
        tell(barrier, device)

    @pl.when(is_owner)
    def _():
        loop(1, owners, lambda shift: greet(owner_device(lax.rem(my_owner + shift, owners))))
        loop(1, groups, lambda shift: greet(counterpart(shift)))
        for core in range(cores - 1):
            loop(0, owners, lambda owner: greet(owner_device(owner, core)))

    for chunk in range(1, chunks):
        loop(0, listed_total, lambda listed: weight_copy(chunk, listed).start())
    for copy in smalls:
        copy.wait()
    live_count = item_count[0]
    kinds = ended[waves - 1]
    kind_of = []
    for listed in range(listed_total):
        label = group_index[0, listed] * n_face + bin_index[0, listed]
        kind_of.append(jnp.where((listed < live_count) & (label < kinds), label, kinds))
    following = [jnp.int32(0)] * (kinds + 1)
    for kind in range(1, kinds + 1):
        following[kind] = following[kind - 1] + sum(
            (of == kind - 1).astype(jnp.int32) for of in kind_of
        )
    picked = [jnp.int32(0) for _ in range(listed_total)]
    for listed in range(listed_total):
        place = jnp.int32(0)
        for kind in range(kinds + 1):
            mine = kind_of[listed] == kind
            place = jnp.where(mine, following[kind], place)
            following[kind] = following[kind] + mine.astype(jnp.int32)
        picked = [jnp.where(place == at, listed, old) for at, old in enumerate(picked)]

    lane = lax.broadcasted_iota(jnp.int32, (1, 128), 1)
    for wave in range(waves):
        lane_at = lane - lax.rem(me, per_row[wave]) * tiles[wave]
        row = jnp.zeros((1, 128), jnp.int32)
        for at in range(sizes[wave]):
            listed = picked[starts[wave] + at]
            label = group_index[0, listed] * n_face + bin_index[0, listed] + 1
            label = jnp.where(listed < live_count, label, 0)
            for copy_at in range(folds[wave]):
                row = jnp.where(lane_at == copy_at * sizes[wave] + at, label, row)
        labels_out[wave] = row

    for copy in loads:
        copy.wait()
    n0, n1, n2 = norms[0:1], norms[1:2], norms[2:3]
    v0, v1, v2 = veloc[0], veloc[1], veloc[2]
    density_now, pressure_now = dens[...], press[...]
    normal_speed = v0 * n0 + v1 * n1 + v2 * n2
    flux = density_now * normal_speed
    thick[...] = (0.5 * (flux[2:] - flux[:-2])).astype(jnp.bfloat16)
    for c, (n, v) in enumerate(((n0, v0), (n1, v1), (n2, v2))):
        load = pressure_now * n + density_now * v * normal_speed
        rate_of[c] = 0.5 * (load[2:] - load[:-2])
        load_of[c] = load[1:-1]

    def prepare(slot):
        h0, h1, h2 = (direction[c, 0, picked[slot]] for c in range(3))
        rate = h0 * rate_of[0] + h1 * rate_of[1] + h2 * rate_of[2]
        radial = h0 * load_of[0] + h1 * load_of[1] + h2 * load_of[2]
        sources[slot] = jnp.concatenate(
            [thick[...], rate.astype(jnp.bfloat16), radial.astype(jnp.bfloat16)], axis=1
        )

    for slot in range(listed_total):
        prepare(slot)

    def compute(chunk, first_wave, last_wave):
        slots = [
            (wave, at) for wave in range(first_wave, last_wave) for at in range(sizes[wave])
        ]
        for first in range(0, len(slots), BATCH):
            batch = slots[first:first + BATCH]
            results = [
                jnp.dot(
                    sources[starts[wave] + at],
                    matrices[chunk][picked[starts[wave] + at]],
                    preferred_element_type=jnp.float32,
                )
                for wave, at in batch
            ]
            for (wave, at), product in zip(batch, results):
                products[wave][chunk, pl.ds(at, steps, stride=sizes[wave]), :] = product

    def await_weights(chunk):
        for listed in range(listed_total):
            weight_copy(chunk, listed).wait()

    def label_copy(owner):
        return pltpu.make_async_remote_copy(
            src_ref=labels_out,
            dst_ref=labels_in.at[me],
            send_sem=label_send,
            recv_sem=label_recv,
            device_id=owner_device(owner),
            device_id_type=MESH,
        )

    def rows_of(wave, owner):
        size = rows * sizes[wave]
        return pl.ds(pl.multiple_of(owner * size, size), size)

    def data_copy(chunk, wave, owner):
        return pltpu.make_async_remote_copy(
            src_ref=products[wave].at[chunk, rows_of(wave, owner)],
            dst_ref=arrived[wave].at[chunk, me],
            send_sem=send_sem.at[chunk, wave],
            recv_sem=recv_sem.at[chunk, wave],
            device_id=owner_device(owner),
            device_id_type=MESH,
        )

    def send_all(copy_of):
        @pl.when(is_owner)
        def _():
            loop(1, owners, lambda shift: copy_of(lax.rem(my_owner + shift, owners)).start())

        @pl.when(jnp.logical_not(is_owner))
        def _():
            loop(0, owners, lambda shift: copy_of(lax.rem(my_owner + shift, owners)).start())

    await_weights(0)
    compute(0, 0, 1)
    pl.semaphore_wait(barrier, jnp.where(is_owner, owners + groups - 2, owners))
    send_all(functools.partial(data_copy, 0, 0))
    send_all(label_copy)

    @pl.when(jnp.logical_not(is_owner))
    def _():
        loop(0, owners, lambda owner: tell(entered, owner_device(owner)))

    compute(0, 1, waves)
    if waves > 1:
        send_all(functools.partial(data_copy, 0, 1))
    for chunk in range(1, chunks):
        await_weights(chunk)
        compute(chunk, 0, min(2, waves))
        for wave in range(min(2, waves)):
            send_all(functools.partial(data_copy, chunk, wave))
    for wave in range(2, waves):
        for chunk in range(chunks):
            if chunk > 0:
                compute(chunk, wave, wave + 1)
            send_all(functools.partial(data_copy, chunk, wave))

    def wait_bytes(ref, sem):
        pltpu.make_async_copy(ref, ref, sem).wait()

    def cell_copy(source, chunk, cell):
        return pltpu.make_async_remote_copy(
            src_ref=source.at[chunk, cell],
            dst_ref=owned.at[chunk, my_group * owners + my_owner],
            send_sem=send_two.at[chunk],
            recv_sem=recv_two.at[chunk],
            device_id=(cell // n_face, cell % n_face),
            device_id_type=MESH,
        )

    def send_cells(source, chunk, first, last):
        def send(cell):
            @pl.when(cell != my_cell)
            def _():
                cell_copy(source, chunk, cell).start()

        for cell in range(first, last):
            send(cell)

        @pl.when((my_cell >= first) & (my_cell < last))
        def _():
            owned[chunk, my_group * owners + my_owner] = source[chunk, my_cell]

    @pl.when(is_owner)
    def _():
        if cores > 1:
            pl.semaphore_wait(entered, members - owners)
        for shift in range(1, groups):
            tell(ready, counterpart(shift))
        labels_in[me] = labels_out[...]
        for chunk in range(chunks):
            for wave in range(waves):
                arrived[wave][chunk, me] = products[wave][chunk, rows_of(wave, my_owner)]
        wait_bytes(labels_in.at[pl.ds(0, members - 1)], label_recv)
        chosen = []
        for wave, (size, fold, tile) in enumerate(zip(sizes, folds, tiles)):
            shape = (fold * total_cells, lanes[wave])
            line = lax.broadcasted_iota(jnp.int32, shape, 0)
            place = lax.rem(lax.broadcasted_iota(jnp.int32, shape, 1), tile) // size
            parts = []
            for first in range(0, members, per_row[wave]):
                keys = jnp.sum(labels_in[first:first + per_row[wave], wave], axis=0)
                keys = keys[:, :lanes[wave]]
                match = (keys + place * total_cells == line + 1) & (keys > 0)
                parts.append(match.astype(jnp.float32).astype(jnp.bfloat16))
            chosen.append(jnp.concatenate(parts + parts, axis=1))

        for wave, (fold, tile) in enumerate(zip(folds, tiles)):
            last = wave == waves - 1
            begin, end = (0, total_cells) if last else ended[wave:wave + 2]
            for chunk in range(chunks):
                wait_bytes(
                    arrived[wave].at[chunk, pl.ds(0, members - 1)], recv_sem.at[chunk, wave]
                )
                values = jnp.concatenate(
                    [
                        arrived[wave][chunk, :, at * tile:(at + 1) * tile, :].reshape(
                            members * tile, part
                        )
                        for at in range(rows // fold)
                    ],
                    axis=1,
                )
                high = values.astype(jnp.bfloat16)
                low = (values - high.astype(jnp.float32)).astype(jnp.bfloat16)
                sums = jnp.dot(
                    chosen[wave],
                    jnp.concatenate([high, low], axis=0),
                    preferred_element_type=jnp.float32,
                )
                for at in range(rows):
                    tile_at, line_at = divmod(at, fold)
                    found = sums[
                        line_at * total_cells:(line_at + 1) * total_cells,
                        tile_at * part:(tile_at + 1) * part,
                    ]
                    if wave > 0:
                        found = found + partial[chunk, at]
                    if last:
                        cells[chunk, :, at, :] = found
                    else:
                        partial[chunk, at] = found
                        first_cells[chunk, begin:end, at, :] = found[begin:end]
                if wave == 0 and chunk == 0 and groups > 1:
                    pl.semaphore_wait(ready, groups - 1)
                if last:
                    send_cells(cells, chunk, kinds, max(kinds, n_face))
                else:
                    send_cells(first_cells, chunk, begin, end)
        for group in range(1, n_obs):
            for chunk in range(chunks):
                send_cells(
                    cells, chunk, max(kinds, group * n_face), (group + 1) * n_face
                )

    senders = groups * owners

    def collect(chunk):
        @pl.when(is_owner)
        def _():
            wait_bytes(owned.at[chunk, pl.ds(0, senders - 1)], recv_two.at[chunk])

        @pl.when(jnp.logical_not(is_owner))
        def _():
            wait_bytes(owned.at[chunk, pl.ds(0, senders)], recv_two.at[chunk])

        for owner in range(owners):
            total = owned[chunk, owner]
            for group in range(1, groups):
                total = total + owned[chunk, group * owners + owner]
            out[owner * rows:(owner + 1) * rows, chunk * part:(chunk + 1) * part] = total

    def drain(count):
        wait_bytes(labels_in.at[pl.ds(0, count)], label_send)
        for chunk in range(chunks):
            for wave in range(waves):
                wait_bytes(arrived[wave].at[chunk, pl.ds(0, count)], send_sem.at[chunk, wave])

    for chunk in range(chunks - 1):
        collect(chunk)

    @pl.when(is_owner)
    def _():
        drain(owners - 1)
        for chunk in range(chunks):
            wait_bytes(cells.at[chunk, pl.ds(0, total_cells - 1)], send_two.at[chunk])

    @pl.when(jnp.logical_not(is_owner))
    def _():
        drain(owners)

    collect(chunks - 1)


def local(
    density, velocity, pressure, normal, direction, weights, bin_index, group_index, item_count
):
    n_face, n_obs = lax.axis_size("face"), lax.axis_size("obs")
    listed_total, depth, width = weights.shape[1:]
    rows, faces = density.shape
    steps = rows - 2
    chunks = max(1, width // 128)
    part = width // chunks
    planes = PLANES if n_obs % PLANES == 0 else 1
    cores = 2 if n_face % 2 == 0 else 1
    members = planes * n_face
    owners = members // cores
    groups = n_obs // planes
    total_cells = n_obs * n_face
    own_rows = steps // owners
    sizes = tuple(listed_total // share for share in SPLIT)
    usable = all(size % SLOT_CAP == 0 and own_rows % max(1, 8 // size) == 0 for size in sizes if size)
    if sum(sizes) != listed_total or min(sizes) == 0 or not usable:
        sizes = (listed_total,)
    waves = len(sizes)
    early = max(1, sum(sizes[:-1]) // SLOT_CAP)
    smem = pl.BlockSpec(memory_space=pltpu.SMEM)
    anywhere = pl.BlockSpec(memory_space=pl.ANY)
    f32, i32 = jnp.float32, jnp.int32
    dma = pltpu.SemaphoreType.DMA
    return pl.pallas_call(
        functools.partial(kernel, n_obs, n_face, planes, cores, chunks, sizes),
        out_shape=pltpu.VMEM((steps, width), f32),
        in_specs=[anywhere] * 3 + [smem] + [anywhere] * 5,
        out_specs=pl.BlockSpec(memory_space=pltpu.VMEM),
        scratch_shapes=[
            pltpu.SMEM((3, 1, listed_total), f32),
            pltpu.SMEM((1, listed_total), i32),
            pltpu.SMEM((1, listed_total), i32),
            pltpu.VMEM((rows, faces), f32),
            pltpu.VMEM((3, rows, faces), f32),
            pltpu.VMEM((rows, faces), f32),
            pltpu.VMEM((3, faces), f32),
            [pltpu.VMEM((listed_total, depth, part), jnp.bfloat16)] * chunks,
            pltpu.VMEM((steps, faces), jnp.bfloat16),
            pltpu.VMEM((3, steps, faces), f32),
            pltpu.VMEM((3, steps, faces), f32),
            pltpu.VMEM((listed_total, steps, depth), jnp.bfloat16),
            [pltpu.VMEM((chunks, steps * size, part), f32) for size in sizes],
            pltpu.VMEM((waves, 1, 128), i32),
            pltpu.VMEM((members, waves, 1, 128), i32),
            [pltpu.VMEM((chunks, members, own_rows * size, part), f32) for size in sizes],
            pltpu.VMEM((chunks, own_rows, total_cells, part), f32),
            pltpu.VMEM((chunks, early, own_rows, part), f32),
            pltpu.VMEM((chunks, total_cells, own_rows, part), f32),
            pltpu.VMEM((chunks, groups * owners, own_rows, part), f32),
            dma((3,)),
            dma((4,)),
            dma((chunks, listed_total)),
            pltpu.SemaphoreType.REGULAR,
            pltpu.SemaphoreType.REGULAR,
            dma,
            dma,
            dma((chunks, waves)),
            dma((chunks, waves)),
            dma((chunks,)),
            dma((chunks,)),
        ],
        compiler_params=pltpu.CompilerParams(
            collective_id=0, has_side_effects=True
        ),
    )(
        jnp.transpose(direction, (2, 0, 1)), bin_index, group_index, item_count,
        density, velocity, pressure, normal, weights,
    )


def solution(mesh):
    placed = (
        P(None, ("obs", "face")),
        P(None, None, ("obs", "face")),
        P(None, ("obs", "face")),
        P(None, ("obs", "face")),
        P(("obs", "face"), None, None),
        P(("obs", "face"), None, None, None),
        P(("obs", "face"), None),
        P(("obs", "face"), None),
        P(("obs", "face")),
    )
    return jax.shard_map(
        local, mesh=mesh, in_specs=placed, out_specs=P("face", "obs"), check_vma=False
    )
```

```python
import functools

import jax
import jax.numpy as jnp
from jax import lax
from jax.experimental import pallas as pl
from jax.experimental.pallas import tpu as pltpu
from jax.sharding import PartitionSpec as P

MESH = pl.DeviceIdType.MESH
BATCH = 8
SLOT_CAP = 2
SPLIT = (4, 4, 2)
PLANES = 1


def loop(first, last, body):
    if last - first <= 8:
        for at in range(first, last):
            body(at)
    else:
        lax.fori_loop(first, last, lambda at, _: (body(at), _)[1], 0)


def kernel(
    n_obs, n_face, planes, cores, chunks, sizes,
    direction_in, bin_in, group_in, item_count,
    density, velocity, pressure, normal, weights,
    out,
    direction, bin_index, group_index,
    dens, veloc, press, norms, matrices, thick, rate_of, load_of, sources,
    products, labels_out, labels_in, arrived, partial, first_cells, cells, owned,
    small_sem, in_sem, weight_sem, entered, ready, label_send, label_recv,
    send_sem, recv_sem, send_two, recv_two,
):
    my_obs, my_face = lax.axis_index("obs"), lax.axis_index("face")
    listed_total, steps = sources.shape[:2]
    part = matrices[0].shape[2]
    groups = n_obs // planes
    members = planes * n_face
    owners_plane = n_face // cores
    owners = planes * owners_plane
    rows = steps // owners
    total_cells = n_obs * n_face
    waves = len(sizes)
    starts = [sum(sizes[:wave]) for wave in range(waves + 1)]
    ended = [start // SLOT_CAP for start in starts]
    folds = [max(1, 8 // size) for size in sizes]
    tiles = [fold * size for fold, size in zip(folds, sizes)]
    lanes = [min(128, members * tile) for tile in tiles]
    per_row = [wide // tile for wide, tile in zip(lanes, tiles)]

    my_group, my_plane = my_obs // planes, lax.rem(my_obs, planes)
    me = my_plane * n_face + my_face
    my_owner = my_plane * owners_plane + my_face // cores
    is_owner = lax.rem(my_face, cores) == cores - 1
    my_cell = my_obs * n_face + my_face

    def member_device(member):
        return (my_group * planes + member // n_face, lax.rem(member, n_face))

    def owner_device(owner, core=cores - 1):
        return (
            my_group * planes + owner // owners_plane,
            lax.rem(owner, owners_plane) * cores + core,
        )

    def counterpart(shift):
        return (lax.rem(my_obs + shift * planes, n_obs), my_face)

    smalls = [
        pltpu.make_async_copy(direction_in, direction, small_sem.at[0]),
        pltpu.make_async_copy(bin_in, bin_index, small_sem.at[1]),
        pltpu.make_async_copy(group_in, group_index, small_sem.at[2]),
    ]
    loads = [
        pltpu.make_async_copy(density, dens, in_sem.at[0]),
        pltpu.make_async_copy(velocity, veloc, in_sem.at[1]),
        pltpu.make_async_copy(pressure, press, in_sem.at[2]),
        pltpu.make_async_copy(normal, norms, in_sem.at[3]),
    ]
    for copy in smalls + loads:
        copy.start()

    def weight_copy(chunk, listed):
        return pltpu.make_async_copy(
            weights.at[0, listed, :, pl.ds(chunk * part, part)],
            matrices[chunk].at[listed],
            weight_sem.at[chunk, listed],
        )

    loop(0, listed_total, lambda listed: weight_copy(0, listed).start())

    barrier = pltpu.get_barrier_semaphore()

    def tell(semaphore, device):
        pl.semaphore_signal(semaphore, inc=1, device_id=device, device_id_type=MESH)

    def greet(device):
        tell(barrier, device)

    @pl.when(is_owner)
    def _():
        loop(1, owners, lambda shift: greet(owner_device(lax.rem(my_owner + shift, owners))))
        loop(1, groups, lambda shift: greet(counterpart(shift)))
        for core in range(cores - 1):
            loop(0, owners, lambda owner: greet(owner_device(owner, core)))

    for chunk in range(1, chunks):
        loop(0, listed_total, lambda listed: weight_copy(chunk, listed).start())
    for copy in smalls:
        copy.wait()
    live_count = item_count[0]
    kinds = ended[waves - 1]
    kind_of = []
    for listed in range(listed_total):
        label = group_index[0, listed] * n_face + bin_index[0, listed]
        kind_of.append(jnp.where((listed < live_count) & (label < kinds), label, kinds))
    following = [jnp.int32(0)] * (kinds + 1)
    for kind in range(1, kinds + 1):
        following[kind] = following[kind - 1] + sum(
            (of == kind - 1).astype(jnp.int32) for of in kind_of
        )
    picked = [jnp.int32(0) for _ in range(listed_total)]
    for listed in range(listed_total):
        place = jnp.int32(0)
        for kind in range(kinds + 1):
            mine = kind_of[listed] == kind
            place = jnp.where(mine, following[kind], place)
            following[kind] = following[kind] + mine.astype(jnp.int32)
        picked = [jnp.where(place == at, listed, old) for at, old in enumerate(picked)]

    lane = lax.broadcasted_iota(jnp.int32, (1, 128), 1)
    for wave in range(waves):
        lane_at = lane - lax.rem(me, per_row[wave]) * tiles[wave]
        row = jnp.zeros((1, 128), jnp.int32)
        for at in range(sizes[wave]):
            listed = picked[starts[wave] + at]
            label = group_index[0, listed] * n_face + bin_index[0, listed] + 1
            label = jnp.where(listed < live_count, label, 0)
            for copy_at in range(folds[wave]):
                row = jnp.where(lane_at == copy_at * sizes[wave] + at, label, row)
        labels_out[wave] = row

    for copy in loads:
        copy.wait()
    n0, n1, n2 = norms[0:1], norms[1:2], norms[2:3]
    v0, v1, v2 = veloc[0], veloc[1], veloc[2]
    density_now, pressure_now = dens[...], press[...]
    normal_speed = v0 * n0 + v1 * n1 + v2 * n2
    flux = density_now * normal_speed
    thick[...] = (0.5 * (flux[2:] - flux[:-2])).astype(jnp.bfloat16)
    for c, (n, v) in enumerate(((n0, v0), (n1, v1), (n2, v2))):
        load = pressure_now * n + density_now * v * normal_speed
        rate_of[c] = 0.5 * (load[2:] - load[:-2])
        load_of[c] = load[1:-1]

    def prepare(slot):
        h0, h1, h2 = (direction[c, 0, picked[slot]] for c in range(3))
        rate = h0 * rate_of[0] + h1 * rate_of[1] + h2 * rate_of[2]
        radial = h0 * load_of[0] + h1 * load_of[1] + h2 * load_of[2]
        sources[slot] = jnp.concatenate(
            [thick[...], rate.astype(jnp.bfloat16), radial.astype(jnp.bfloat16)], axis=1
        )

    for slot in range(listed_total):
        prepare(slot)

    def compute(chunk, first_wave, last_wave):
        slots = [
            (wave, at) for wave in range(first_wave, last_wave) for at in range(sizes[wave])
        ]
        for first in range(0, len(slots), BATCH):
            batch = slots[first:first + BATCH]
            results = [
                jnp.dot(
                    sources[starts[wave] + at],
                    matrices[chunk][picked[starts[wave] + at]],
                    preferred_element_type=jnp.float32,
                )
                for wave, at in batch
            ]
            for (wave, at), product in zip(batch, results):
                products[wave][chunk, pl.ds(at, steps, stride=sizes[wave]), :] = product

    def await_weights(chunk):
        for listed in range(listed_total):
            weight_copy(chunk, listed).wait()

    def label_copy(owner):
        return pltpu.make_async_remote_copy(
            src_ref=labels_out,
            dst_ref=labels_in.at[me],
            send_sem=label_send,
            recv_sem=label_recv,
            device_id=owner_device(owner),
            device_id_type=MESH,
        )

    def rows_of(wave, owner):
        size = rows * sizes[wave]
        return pl.ds(pl.multiple_of(owner * size, size), size)

    def data_copy(chunk, wave, owner):
        return pltpu.make_async_remote_copy(
            src_ref=products[wave].at[chunk, rows_of(wave, owner)],
            dst_ref=arrived[wave].at[chunk, me],
            send_sem=send_sem.at[chunk, wave],
            recv_sem=recv_sem.at[chunk, wave],
            device_id=owner_device(owner),
            device_id_type=MESH,
        )

    def send_all(copy_of):
        @pl.when(is_owner)
        def _():
            loop(1, owners, lambda shift: copy_of(lax.rem(my_owner + shift, owners)).start())

        @pl.when(jnp.logical_not(is_owner))
        def _():
            loop(0, owners, lambda shift: copy_of(lax.rem(my_owner + shift, owners)).start())

    await_weights(0)
    compute(0, 0, 1)
    pl.semaphore_wait(barrier, jnp.where(is_owner, owners + groups - 2, owners))
    send_all(functools.partial(data_copy, 0, 0))
    send_all(label_copy)

    @pl.when(jnp.logical_not(is_owner))
    def _():
        loop(0, owners, lambda owner: tell(entered, owner_device(owner)))

    compute(0, 1, waves)
    for chunk in range(1, chunks):
        await_weights(chunk)
        compute(chunk, 0, 1)
        send_all(functools.partial(data_copy, chunk, 0))
    if waves > 1:
        send_all(functools.partial(data_copy, 0, 1))
    for chunk in range(1, chunks):
        compute(chunk, 1, waves)
    for wave in range(1, waves):
        for chunk in range(chunks):
            if (wave, chunk) != (1, 0):
                send_all(functools.partial(data_copy, chunk, wave))

    def wait_bytes(ref, sem):
        pltpu.make_async_copy(ref, ref, sem).wait()

    def cell_copy(source, chunk, cell):
        return pltpu.make_async_remote_copy(
            src_ref=source.at[chunk, cell],
            dst_ref=owned.at[chunk, my_group * owners + my_owner],
            send_sem=send_two.at[chunk],
            recv_sem=recv_two.at[chunk],
            device_id=(cell // n_face, cell % n_face),
            device_id_type=MESH,
        )

    def send_cells(source, chunk, first, last):
        def send(cell):
            @pl.when(cell != my_cell)
            def _():
                cell_copy(source, chunk, cell).start()

        if last <= min(n_face, 8):
            for core in reversed(range(cores)):
                for cell in range(first, last):
                    if cell % cores == core:
                        send(cell)
        else:
            loop(first, last, send)

        @pl.when((my_cell >= first) & (my_cell < last))
        def _():
            owned[chunk, my_group * owners + my_owner] = source[chunk, my_cell]

    @pl.when(is_owner)
    def _():
        if cores > 1:
            pl.semaphore_wait(entered, members - owners)
        for shift in range(1, groups):
            tell(ready, counterpart(shift))
        labels_in[me] = labels_out[...]
        for chunk in range(chunks):
            for wave in range(waves):
                arrived[wave][chunk, me] = products[wave][chunk, rows_of(wave, my_owner)]
        wait_bytes(labels_in.at[pl.ds(0, members - 1)], label_recv)
        chosen = []
        for wave, (size, fold, tile) in enumerate(zip(sizes, folds, tiles)):
            shape = (fold * total_cells, lanes[wave])
            line = lax.broadcasted_iota(jnp.int32, shape, 0)
            place = lax.rem(lax.broadcasted_iota(jnp.int32, shape, 1), tile) // size
            parts = []
            for first in range(0, members, per_row[wave]):
                keys = jnp.sum(labels_in[first:first + per_row[wave], wave], axis=0)
                keys = keys[:, :lanes[wave]]
                match = (keys + place * total_cells == line + 1) & (keys > 0)
                parts.append(match.astype(jnp.float32).astype(jnp.bfloat16))
            chosen.append(jnp.concatenate(parts + parts, axis=1))

        for wave, (fold, tile) in enumerate(zip(folds, tiles)):
            last = wave == waves - 1
            begin, end = (0, total_cells) if last else ended[wave:wave + 2]
            for chunk in range(chunks):
                wait_bytes(
                    arrived[wave].at[chunk, pl.ds(0, members - 1)], recv_sem.at[chunk, wave]
                )
                values = jnp.concatenate(
                    [
                        arrived[wave][chunk, :, at * tile:(at + 1) * tile, :].reshape(
                            members * tile, part
                        )
                        for at in range(rows // fold)
                    ],
                    axis=1,
                )
                high = values.astype(jnp.bfloat16)
                low = (values - high.astype(jnp.float32)).astype(jnp.bfloat16)
                sums = jnp.dot(
                    chosen[wave],
                    jnp.concatenate([high, low], axis=0),
                    preferred_element_type=jnp.float32,
                )
                for at in range(rows):
                    tile_at, line_at = divmod(at, fold)
                    found = sums[
                        line_at * total_cells:(line_at + 1) * total_cells,
                        tile_at * part:(tile_at + 1) * part,
                    ]
                    if wave > 0:
                        found = found + partial[chunk, at]
                    if last:
                        cells[chunk, :, at, :] = found
                    else:
                        partial[chunk, at] = found
                        first_cells[chunk, begin:end, at, :] = found[begin:end]
                if wave == 0 and chunk == 0 and groups > 1:
                    pl.semaphore_wait(ready, groups - 1)
                if last:
                    send_cells(cells, chunk, kinds, max(kinds, n_face))
                else:
                    send_cells(first_cells, chunk, begin, end)
        for group in range(1, n_obs):
            for chunk in range(chunks):
                send_cells(
                    cells, chunk, max(kinds, group * n_face), (group + 1) * n_face
                )

    senders = groups * owners

    def collect(chunk):
        @pl.when(is_owner)
        def _():
            wait_bytes(owned.at[chunk, pl.ds(0, senders - 1)], recv_two.at[chunk])

        @pl.when(jnp.logical_not(is_owner))
        def _():
            wait_bytes(owned.at[chunk, pl.ds(0, senders)], recv_two.at[chunk])

        for owner in range(owners):
            total = owned[chunk, owner]
            for group in range(1, groups):
                total = total + owned[chunk, group * owners + owner]
            out[owner * rows:(owner + 1) * rows, chunk * part:(chunk + 1) * part] = total

    def drain(count):
        wait_bytes(labels_in.at[pl.ds(0, count)], label_send)
        for chunk in range(chunks):
            for wave in range(waves):
                wait_bytes(arrived[wave].at[chunk, pl.ds(0, count)], send_sem.at[chunk, wave])

    for chunk in range(chunks - 1):
        collect(chunk)

    @pl.when(is_owner)
    def _():
        drain(owners - 1)
        for chunk in range(chunks):
            wait_bytes(cells.at[chunk, pl.ds(0, total_cells - 1)], send_two.at[chunk])

    @pl.when(jnp.logical_not(is_owner))
    def _():
        drain(owners)

    collect(chunks - 1)


def local(
    density, velocity, pressure, normal, direction, weights, bin_index, group_index, item_count
):
    n_face, n_obs = lax.axis_size("face"), lax.axis_size("obs")
    listed_total, depth, width = weights.shape[1:]
    rows, faces = density.shape
    steps = rows - 2
    chunks = max(1, width // 128)
    part = width // chunks
    planes = PLANES if n_obs % PLANES == 0 else 1
    cores = 2 if n_face % 2 == 0 else 1
    members = planes * n_face
    owners = members // cores
    groups = n_obs // planes
    total_cells = n_obs * n_face
    own_rows = steps // owners
    sizes = tuple(listed_total // share for share in SPLIT)
    usable = all(size % SLOT_CAP == 0 and own_rows % max(1, 8 // size) == 0 for size in sizes if size)
    if sum(sizes) != listed_total or min(sizes) == 0 or not usable:
        sizes = (listed_total,)
    waves = len(sizes)
    early = max(1, sum(sizes[:-1]) // SLOT_CAP)
    smem = pl.BlockSpec(memory_space=pltpu.SMEM)
    anywhere = pl.BlockSpec(memory_space=pl.ANY)
    f32, i32 = jnp.float32, jnp.int32
    dma = pltpu.SemaphoreType.DMA
    return pl.pallas_call(
        functools.partial(kernel, n_obs, n_face, planes, cores, chunks, sizes),
        out_shape=pltpu.VMEM((steps, width), f32),
        in_specs=[anywhere] * 3 + [smem] + [anywhere] * 5,
        out_specs=pl.BlockSpec(memory_space=pltpu.VMEM),
        scratch_shapes=[
            pltpu.SMEM((3, 1, listed_total), f32),
            pltpu.SMEM((1, listed_total), i32),
            pltpu.SMEM((1, listed_total), i32),
            pltpu.VMEM((rows, faces), f32),
            pltpu.VMEM((3, rows, faces), f32),
            pltpu.VMEM((rows, faces), f32),
            pltpu.VMEM((3, faces), f32),
            [pltpu.VMEM((listed_total, depth, part), jnp.bfloat16)] * chunks,
            pltpu.VMEM((steps, faces), jnp.bfloat16),
            pltpu.VMEM((3, steps, faces), f32),
            pltpu.VMEM((3, steps, faces), f32),
            pltpu.VMEM((listed_total, steps, depth), jnp.bfloat16),
            [pltpu.VMEM((chunks, steps * size, part), f32) for size in sizes],
            pltpu.VMEM((waves, 1, 128), i32),
            pltpu.VMEM((members, waves, 1, 128), i32),
            [pltpu.VMEM((chunks, members, own_rows * size, part), f32) for size in sizes],
            pltpu.VMEM((chunks, own_rows, total_cells, part), f32),
            pltpu.VMEM((chunks, early, own_rows, part), f32),
            pltpu.VMEM((chunks, total_cells, own_rows, part), f32),
            pltpu.VMEM((chunks, groups * owners, own_rows, part), f32),
            dma((3,)),
            dma((4,)),
            dma((chunks, listed_total)),
            pltpu.SemaphoreType.REGULAR,
            pltpu.SemaphoreType.REGULAR,
            dma,
            dma,
            dma((chunks, waves)),
            dma((chunks, waves)),
            dma((chunks,)),
            dma((chunks,)),
        ],
        compiler_params=pltpu.CompilerParams(
            collective_id=0, has_side_effects=True
        ),
    )(
        jnp.transpose(direction, (2, 0, 1)), bin_index, group_index, item_count,
        density, velocity, pressure, normal, weights,
    )


def solution(mesh):
    placed = (
        P(None, ("obs", "face")),
        P(None, None, ("obs", "face")),
        P(None, ("obs", "face")),
        P(None, ("obs", "face")),
        P(("obs", "face"), None, None),
        P(("obs", "face"), None, None, None),
        P(("obs", "face"), None),
        P(("obs", "face"), None),
        P(("obs", "face")),
    )
    return jax.shard_map(
        local, mesh=mesh, in_specs=placed, out_specs=P("face", "obs"), check_vma=False
    )
```

```python
import functools

import jax
import jax.numpy as jnp
from jax import lax
from jax.experimental import pallas as pl
from jax.experimental.pallas import tpu as pltpu
from jax.sharding import PartitionSpec as P

MESH = pl.DeviceIdType.MESH
BATCH = 8
SLOT_CAP = 2
SPLIT = (4, 4, 2)
PLANES = 1


def loop(first, last, body):
    if last - first <= 8:
        for at in range(first, last):
            body(at)
    else:
        lax.fori_loop(first, last, lambda at, _: (body(at), _)[1], 0)


def kernel(
    n_obs, n_face, planes, cores, chunks, sizes,
    direction_in, bin_in, group_in, item_count,
    density, velocity, pressure, normal, weights,
    out,
    direction, bin_index, group_index,
    dens, veloc, press, norms, matrices, thick, rate_of, load_of, sources,
    products, labels_out, labels_in, arrived, partial, first_cells, cells, owned,
    small_sem, in_sem, weight_sem, entered, ready, label_send, label_recv,
    send_sem, recv_sem, send_two, recv_two,
):
    my_obs, my_face = lax.axis_index("obs"), lax.axis_index("face")
    listed_total, steps = sources.shape[:2]
    part = matrices[0].shape[2]
    groups = n_obs // planes
    members = planes * n_face
    owners_plane = n_face // cores
    owners = planes * owners_plane
    rows = steps // owners
    total_cells = n_obs * n_face
    waves = len(sizes)
    starts = [sum(sizes[:wave]) for wave in range(waves + 1)]
    ended = [start // SLOT_CAP for start in starts]
    folds = [max(1, 8 // size) for size in sizes]
    tiles = [fold * size for fold, size in zip(folds, sizes)]
    lanes = [min(128, members * tile) for tile in tiles]
    per_row = [wide // tile for wide, tile in zip(lanes, tiles)]

    my_group, my_plane = my_obs // planes, lax.rem(my_obs, planes)
    me = my_plane * n_face + my_face
    my_owner = my_plane * owners_plane + my_face // cores
    is_owner = lax.rem(my_face, cores) == cores - 1
    my_cell = my_obs * n_face + my_face

    def member_device(member):
        return (my_group * planes + member // n_face, lax.rem(member, n_face))

    def owner_device(owner, core=cores - 1):
        return (
            my_group * planes + owner // owners_plane,
            lax.rem(owner, owners_plane) * cores + core,
        )

    def counterpart(shift):
        return (lax.rem(my_obs + shift * planes, n_obs), my_face)

    smalls = [
        pltpu.make_async_copy(direction_in, direction, small_sem.at[0]),
        pltpu.make_async_copy(bin_in, bin_index, small_sem.at[1]),
        pltpu.make_async_copy(group_in, group_index, small_sem.at[2]),
    ]
    loads = [
        pltpu.make_async_copy(density, dens, in_sem.at[0]),
        pltpu.make_async_copy(velocity, veloc, in_sem.at[1]),
        pltpu.make_async_copy(pressure, press, in_sem.at[2]),
        pltpu.make_async_copy(normal, norms, in_sem.at[3]),
    ]
    for copy in smalls + loads:
        copy.start()

    def weight_copy(chunk, listed):
        return pltpu.make_async_copy(
            weights.at[0, listed, :, pl.ds(chunk * part, part)],
            matrices[chunk].at[listed],
            weight_sem.at[chunk, listed],
        )

    loop(0, listed_total, lambda listed: weight_copy(0, listed).start())

    barrier = pltpu.get_barrier_semaphore()

    def tell(semaphore, device):
        pl.semaphore_signal(semaphore, inc=1, device_id=device, device_id_type=MESH)

    def greet(device):
        tell(barrier, device)

    @pl.when(is_owner)
    def _():
        loop(1, owners, lambda shift: greet(owner_device(lax.rem(my_owner + shift, owners))))
        loop(1, groups, lambda shift: greet(counterpart(shift)))
        for core in range(cores - 1):
            loop(0, owners, lambda owner: greet(owner_device(owner, core)))

    for chunk in range(1, chunks):
        loop(0, listed_total, lambda listed: weight_copy(chunk, listed).start())
    for copy in smalls:
        copy.wait()
    live_count = item_count[0]
    kinds = ended[waves - 1]
    kind_of = []
    for listed in range(listed_total):
        label = group_index[0, listed] * n_face + bin_index[0, listed]
        kind_of.append(jnp.where((listed < live_count) & (label < kinds), label, kinds))
    following = [jnp.int32(0)] * (kinds + 1)
    for kind in range(1, kinds + 1):
        following[kind] = following[kind - 1] + sum(
            (of == kind - 1).astype(jnp.int32) for of in kind_of
        )
    picked = [jnp.int32(0) for _ in range(listed_total)]
    for listed in range(listed_total):
        place = jnp.int32(0)
        for kind in range(kinds + 1):
            mine = kind_of[listed] == kind
            place = jnp.where(mine, following[kind], place)
            following[kind] = following[kind] + mine.astype(jnp.int32)
        picked = [jnp.where(place == at, listed, old) for at, old in enumerate(picked)]

    lane = lax.broadcasted_iota(jnp.int32, (1, 128), 1)
    for wave in range(waves):
        lane_at = lane - lax.rem(me, per_row[wave]) * tiles[wave]
        row = jnp.zeros((1, 128), jnp.int32)
        for at in range(sizes[wave]):
            listed = picked[starts[wave] + at]
            label = group_index[0, listed] * n_face + bin_index[0, listed] + 1
            label = jnp.where(listed < live_count, label, 0)
            for copy_at in range(folds[wave]):
                row = jnp.where(lane_at == copy_at * sizes[wave] + at, label, row)
        labels_out[wave] = row

    for copy in loads:
        copy.wait()
    n0, n1, n2 = norms[0:1], norms[1:2], norms[2:3]
    v0, v1, v2 = veloc[0], veloc[1], veloc[2]
    density_now, pressure_now = dens[...], press[...]
    normal_speed = v0 * n0 + v1 * n1 + v2 * n2
    flux = density_now * normal_speed
    thick[...] = (0.5 * (flux[2:] - flux[:-2])).astype(jnp.bfloat16)
    for c, (n, v) in enumerate(((n0, v0), (n1, v1), (n2, v2))):
        load = pressure_now * n + density_now * v * normal_speed
        rate_of[c] = 0.5 * (load[2:] - load[:-2])
        load_of[c] = load[1:-1]

    def prepare(slot):
        h0, h1, h2 = (direction[c, 0, picked[slot]] for c in range(3))
        rate = h0 * rate_of[0] + h1 * rate_of[1] + h2 * rate_of[2]
        radial = h0 * load_of[0] + h1 * load_of[1] + h2 * load_of[2]
        sources[slot] = jnp.concatenate(
            [thick[...], rate.astype(jnp.bfloat16), radial.astype(jnp.bfloat16)], axis=1
        )

    for slot in range(listed_total):
        prepare(slot)

    def compute(chunk, first_wave, last_wave):
        slots = [
            (wave, at) for wave in range(first_wave, last_wave) for at in range(sizes[wave])
        ]
        for first in range(0, len(slots), BATCH):
            batch = slots[first:first + BATCH]
            results = [
                jnp.dot(
                    sources[starts[wave] + at],
                    matrices[chunk][picked[starts[wave] + at]],
                    preferred_element_type=jnp.float32,
                )
                for wave, at in batch
            ]
            for (wave, at), product in zip(batch, results):
                products[wave][chunk, pl.ds(at, steps, stride=sizes[wave]), :] = product

    def await_weights(chunk):
        for listed in range(listed_total):
            weight_copy(chunk, listed).wait()

    def label_copy(owner):
        return pltpu.make_async_remote_copy(
            src_ref=labels_out,
            dst_ref=labels_in.at[me],
            send_sem=label_send,
            recv_sem=label_recv,
            device_id=owner_device(owner),
            device_id_type=MESH,
        )

    def rows_of(wave, owner):
        size = rows * sizes[wave]
        return pl.ds(pl.multiple_of(owner * size, size), size)

    def data_copy(chunk, wave, owner):
        return pltpu.make_async_remote_copy(
            src_ref=products[wave].at[chunk, rows_of(wave, owner)],
            dst_ref=arrived[wave].at[chunk, me],
            send_sem=send_sem.at[chunk, wave],
            recv_sem=recv_sem.at[chunk, wave],
            device_id=owner_device(owner),
            device_id_type=MESH,
        )

    def send_all(copy_of):
        @pl.when(is_owner)
        def _():
            loop(1, owners, lambda shift: copy_of(lax.rem(my_owner + shift, owners)).start())

        @pl.when(jnp.logical_not(is_owner))
        def _():
            loop(0, owners, lambda shift: copy_of(lax.rem(my_owner + shift, owners)).start())

    await_weights(0)
    compute(0, 0, 1)
    pl.semaphore_wait(barrier, jnp.where(is_owner, owners + groups - 2, owners))
    send_all(functools.partial(data_copy, 0, 0))
    send_all(label_copy)

    @pl.when(jnp.logical_not(is_owner))
    def _():
        loop(0, owners, lambda owner: tell(entered, owner_device(owner)))

    compute(0, 1, waves)
    if waves > 1:
        send_all(functools.partial(data_copy, 0, 1))
    for chunk in range(1, chunks):
        await_weights(chunk)
        compute(chunk, 0, min(2, waves))
        for wave in range(min(2, waves)):
            send_all(functools.partial(data_copy, chunk, wave))
    for wave in range(2, waves):
        for chunk in range(chunks):
            if chunk > 0:
                compute(chunk, wave, wave + 1)
            send_all(functools.partial(data_copy, chunk, wave))

    def wait_bytes(ref, sem):
        pltpu.make_async_copy(ref, ref, sem).wait()

    def cell_copy(source, chunk, cell):
        return pltpu.make_async_remote_copy(
            src_ref=source.at[chunk, cell],
            dst_ref=owned.at[chunk, my_group * owners + my_owner],
            send_sem=send_two.at[chunk],
            recv_sem=recv_two.at[chunk],
            device_id=(cell // n_face, cell % n_face),
            device_id_type=MESH,
        )

    def send_cells(source, chunk, first, last):
        def send(cell):
            @pl.when(cell != my_cell)
            def _():
                cell_copy(source, chunk, cell).start()

        if last <= min(n_face, 8):
            for core in reversed(range(cores)):
                for cell in range(first, last):
                    if cell % cores == core:
                        send(cell)
        else:
            loop(first, last, send)

        @pl.when((my_cell >= first) & (my_cell < last))
        def _():
            owned[chunk, my_group * owners + my_owner] = source[chunk, my_cell]

    @pl.when(is_owner)
    def _():
        if cores > 1:
            pl.semaphore_wait(entered, members - owners)
        for shift in range(1, groups):
            tell(ready, counterpart(shift))
        labels_in[me] = labels_out[...]
        for chunk in range(chunks):
            for wave in range(waves):
                arrived[wave][chunk, me] = products[wave][chunk, rows_of(wave, my_owner)]
        wait_bytes(labels_in.at[pl.ds(0, members - 1)], label_recv)
        chosen = []
        for wave, (size, fold, tile) in enumerate(zip(sizes, folds, tiles)):
            shape = (fold * total_cells, lanes[wave])
            line = lax.broadcasted_iota(jnp.int32, shape, 0)
            place = lax.rem(lax.broadcasted_iota(jnp.int32, shape, 1), tile) // size
            parts = []
            for first in range(0, members, per_row[wave]):
                keys = jnp.sum(labels_in[first:first + per_row[wave], wave], axis=0)
                keys = keys[:, :lanes[wave]]
                match = (keys + place * total_cells == line + 1) & (keys > 0)
                parts.append(match.astype(jnp.float32).astype(jnp.bfloat16))
            chosen.append(jnp.concatenate(parts + parts, axis=1))

        for wave, (fold, tile) in enumerate(zip(folds, tiles)):
            last = wave == waves - 1
            begin, end = (0, total_cells) if last else ended[wave:wave + 2]
            for chunk in range(chunks):
                wait_bytes(
                    arrived[wave].at[chunk, pl.ds(0, members - 1)], recv_sem.at[chunk, wave]
                )
                values = jnp.concatenate(
                    [
                        arrived[wave][chunk, :, at * tile:(at + 1) * tile, :].reshape(
                            members * tile, part
                        )
                        for at in range(rows // fold)
                    ],
                    axis=1,
                )
                high = values.astype(jnp.bfloat16)
                low = (values - high.astype(jnp.float32)).astype(jnp.bfloat16)
                sums = jnp.dot(
                    chosen[wave],
                    jnp.concatenate([high, low], axis=0),
                    preferred_element_type=jnp.float32,
                )
                for at in range(rows):
                    tile_at, line_at = divmod(at, fold)
                    found = sums[
                        line_at * total_cells:(line_at + 1) * total_cells,
                        tile_at * part:(tile_at + 1) * part,
                    ]
                    if wave > 0:
                        found = found + partial[chunk, at]
                    if last:
                        cells[chunk, :, at, :] = found
                    else:
                        partial[chunk, at] = found
                        first_cells[chunk, begin:end, at, :] = found[begin:end]
                if wave == 0 and chunk == 0 and groups > 1:
                    pl.semaphore_wait(ready, groups - 1)
                if last:
                    send_cells(cells, chunk, kinds, max(kinds, n_face))
                else:
                    send_cells(first_cells, chunk, begin, end)
        for group in range(1, n_obs):
            for chunk in range(chunks):
                send_cells(
                    cells, chunk, max(kinds, group * n_face), (group + 1) * n_face
                )

    senders = groups * owners

    def collect(chunk):
        @pl.when(is_owner)
        def _():
            wait_bytes(owned.at[chunk, pl.ds(0, senders - 1)], recv_two.at[chunk])

        @pl.when(jnp.logical_not(is_owner))
        def _():
            wait_bytes(owned.at[chunk, pl.ds(0, senders)], recv_two.at[chunk])

        for owner in range(owners):
            total = owned[chunk, owner]
            for group in range(1, groups):
                total = total + owned[chunk, group * owners + owner]
            out[owner * rows:(owner + 1) * rows, chunk * part:(chunk + 1) * part] = total

    def drain(count):
        wait_bytes(labels_in.at[pl.ds(0, count)], label_send)
        for chunk in range(chunks):
            for wave in range(waves):
                wait_bytes(arrived[wave].at[chunk, pl.ds(0, count)], send_sem.at[chunk, wave])

    for chunk in range(chunks - 1):
        collect(chunk)

    @pl.when(is_owner)
    def _():
        drain(owners - 1)
        for chunk in range(chunks):
            wait_bytes(cells.at[chunk, pl.ds(0, total_cells - 1)], send_two.at[chunk])

    @pl.when(jnp.logical_not(is_owner))
    def _():
        drain(owners)

    collect(chunks - 1)


def local(
    density, velocity, pressure, normal, direction, weights, bin_index, group_index, item_count
):
    n_face, n_obs = lax.axis_size("face"), lax.axis_size("obs")
    listed_total, depth, width = weights.shape[1:]
    rows, faces = density.shape
    steps = rows - 2
    chunks = max(1, width // 128)
    part = width // chunks
    planes = PLANES if n_obs % PLANES == 0 else 1
    cores = 2 if n_face % 2 == 0 else 1
    members = planes * n_face
    owners = members // cores
    groups = n_obs // planes
    total_cells = n_obs * n_face
    own_rows = steps // owners
    sizes = tuple(listed_total // share for share in SPLIT)
    usable = all(size % SLOT_CAP == 0 and own_rows % max(1, 8 // size) == 0 for size in sizes if size)
    if sum(sizes) != listed_total or min(sizes) == 0 or not usable:
        sizes = (listed_total,)
    waves = len(sizes)
    early = max(1, sum(sizes[:-1]) // SLOT_CAP)
    smem = pl.BlockSpec(memory_space=pltpu.SMEM)
    anywhere = pl.BlockSpec(memory_space=pl.ANY)
    f32, i32 = jnp.float32, jnp.int32
    dma = pltpu.SemaphoreType.DMA
    return pl.pallas_call(
        functools.partial(kernel, n_obs, n_face, planes, cores, chunks, sizes),
        out_shape=pltpu.VMEM((steps, width), f32),
        in_specs=[anywhere] * 3 + [smem] + [anywhere] * 5,
        out_specs=pl.BlockSpec(memory_space=pltpu.VMEM),
        scratch_shapes=[
            pltpu.SMEM((3, 1, listed_total), f32),
            pltpu.SMEM((1, listed_total), i32),
            pltpu.SMEM((1, listed_total), i32),
            pltpu.VMEM((rows, faces), f32),
            pltpu.VMEM((3, rows, faces), f32),
            pltpu.VMEM((rows, faces), f32),
            pltpu.VMEM((3, faces), f32),
            [pltpu.VMEM((listed_total, depth, part), jnp.bfloat16)] * chunks,
            pltpu.VMEM((steps, faces), jnp.bfloat16),
            pltpu.VMEM((3, steps, faces), f32),
            pltpu.VMEM((3, steps, faces), f32),
            pltpu.VMEM((listed_total, steps, depth), jnp.bfloat16),
            [pltpu.VMEM((chunks, steps * size, part), f32) for size in sizes],
            pltpu.VMEM((waves, 1, 128), i32),
            pltpu.VMEM((members, waves, 1, 128), i32),
            [pltpu.VMEM((chunks, members, own_rows * size, part), f32) for size in sizes],
            pltpu.VMEM((chunks, own_rows, total_cells, part), f32),
            pltpu.VMEM((chunks, early, own_rows, part), f32),
            pltpu.VMEM((chunks, total_cells, own_rows, part), f32),
            pltpu.VMEM((chunks, groups * owners, own_rows, part), f32),
            dma((3,)),
            dma((4,)),
            dma((chunks, listed_total)),
            pltpu.SemaphoreType.REGULAR,
            pltpu.SemaphoreType.REGULAR,
            dma,
            dma,
            dma((chunks, waves)),
            dma((chunks, waves)),
            dma((chunks,)),
            dma((chunks,)),
        ],
        compiler_params=pltpu.CompilerParams(
            collective_id=0, has_side_effects=True
        ),
    )(
        jnp.transpose(direction, (2, 0, 1)), bin_index, group_index, item_count,
        density, velocity, pressure, normal, weights,
    )


def solution(mesh):
    placed = (
        P(None, ("obs", "face")),
        P(None, None, ("obs", "face")),
        P(None, ("obs", "face")),
        P(None, ("obs", "face")),
        P(("obs", "face"), None, None),
        P(("obs", "face"), None, None, None),
        P(("obs", "face"), None),
        P(("obs", "face"), None),
        P(("obs", "face")),
    )
    return jax.shard_map(
        local, mesh=mesh, in_specs=placed, out_specs=P("face", "obs"), check_vma=False
    )
```
